768 devices in a mesh: ep: 32 (over y, x), dp: 2 (over core), tp: 12 (over z).
Axes of the slice: x: 4, y: 8, z: 12, core: 2. Of those that a mesh axis runs over, the one named last changes fastest.
Arguments:
- tokens: bfloat16 [1536, 7168], P(('ep', 'dp')), may hold values from -6 to 6
- expert_ids: int32 [1536, 8], P(('ep', 'dp')), may hold values from 0 to 31, all different within a row; in each aligned block of 24 rows (0 to 23, 24 to 47, ...) at most 8 rows name the same one
- route_weight: float32 [1536, 8], P(('ep', 'dp')), may hold values from 0.1 to 0.6
- gate_weight: bfloat16 [32, 7168, 1536], P('ep', None, 'tp'), may hold values from -0.0625 to 0.0625
- up_weight: bfloat16 [32, 7168, 1536], P('ep', None, 'tp'), may hold values from -0.0625 to 0.0625
- down_weight: bfloat16 [32, 1536, 7168], P('ep', 'tp'), may hold values from -0.15625 to 0.15625
Outputs:
- moe_out: bfloat16 [1536, 7168], P(('ep', 'dp', 'tp'))
The draws below stay inside these ranges and needn't reach their ends.
Inputs may be any that keep to these rules, and one draw needn't show every extreme that they name: `expert_ids`: each row names 8 different experts. In every aligned block of 24 rows no expert is named by more than 8 rows, a bound that some block reaches.
All inputs are finite; a program needn't handle non-finite values.
Results may differ from the reference program's by a relative error of at most 0.0049.
Values may be sent and summed in bfloat16 or wider, within the bound.
No kernel may reach another device: no remote copies, remote signals or barrier semaphores. Data moves between devices by JAX's collectives and lax.ppermute only.
A program may use at most 64 MiB of HBM per device.

```python
import math
import jax
import jax.numpy as jnp
import numpy as np
from jax import lax

D = 7168
FF = 1536
TOP = 8
EXPERTS = 32
TOK_DEV = 24
MOST = 8
TOKENS = 1536
N_TP = 12


def shard_levels(stream_key, dims, shards, low, high):
    def one(axis_at, shards_of):
        heights = jax.random.uniform(jax.random.fold_in(jax.random.fold_in(stream_key, 6), axis_at), (shards_of,), jnp.float32, low / len(shards), high / len(shards))
        return jnp.repeat(jnp.exp(heights), dims[axis_at] // shards_of).reshape((-1,) + (1,) * (len(dims) - axis_at - 1))

    level = one(*shards[0])
    for cut in shards[1:]:
        level = level * one(*cut)
    return level


def routed_block(rng, own, number, rows, count, top, reach, lean):
    ranking = jax.random.permutation(rng, count)
    crowded, usual = load_shares(count, rows * top, reach, lean, True), load_shares(count, rows * top, reach, lean, False)
    places = jnp.arange(count)

    def named(lengths, turn):
        used = int((lengths > 0).sum())
        fixed = max(1, used // 4)
        passed = fixed + (places - fixed + turn * (used - fixed)) % max(1, count - fixed)
        return jnp.zeros((count,), jnp.int32).at[ranking[jnp.where(places < fixed, places, passed)]].set(jnp.asarray(lengths, jnp.int32))

    lengths = jnp.where(number % 4 == 0, named(crowded, number // 4), named(usual, number - number // 4 - 1))
    mixed = jax.random.permutation(jax.random.fold_in(own, 3), count)
    giver, taker = mixed[0:count // 2 * 2:2], mixed[1:count // 2 * 2:2]
    room = jnp.minimum(lengths[giver] - 1, reach - lengths[taker]) // 2
    room = jnp.where((giver == ranking[0]) | (taker == ranking[0]) | (lengths[taker] == 0), 0, jnp.maximum(room, 0))
    passed = jax.random.randint(jax.random.fold_in(own, 4), (count // 2,), 0, 1 << 20) % (room + 1)
    lengths = lengths.at[giver].add(-passed).at[taker].add(passed)
    members = jnp.searchsorted(jnp.cumsum(lengths), jnp.arange(rows * top), side="right").astype(jnp.int32)
    grid = members.reshape(top, rows).T
    grid = grid[jax.random.permutation(jax.random.fold_in(own, 1), rows)]
    turn = jax.random.randint(jax.random.fold_in(own, 2), (rows, 1), 0, top)
    return jnp.take_along_axis(grid, (jnp.arange(top)[None, :] + turn) % top, axis=1)


def load_shares(count, total, most, slope, full):
    portions = [(1 << 20) // math.isqrt(grade ** slope) + 1 for grade in range(1, count + 1)]
    largest = most if full else min(most, max(-(-total // count), total * portions[0] // sum(portions)))
    least = 1 if total - largest >= count - 1 else 0
    counts, surplus = [largest] + [least] * (count - 1), total - largest - least * (count - 1)
    while surplus > 0:
        candidates = [i for i in range(1, count) if counts[i] < largest] or [i for i in range(1, count) if counts[i] < most]
        pool, left = sum([portions[i] for i in candidates]), surplus
        for i in candidates:
            addition = min(most - counts[i], max(1, left * portions[i] // pool), surplus)
            counts[i] = counts[i] + addition
            surplus = surplus - addition
    return np.array(counts)


def noise(rng, dims, width, limit, cuts=(), held_as=jnp.bfloat16):
    gain = shard_levels(rng, dims, cuts, -0.22, 0.18) if cuts else 1.0
    result = jax.random.normal(rng, dims, jnp.float32) * width * gain
    return jnp.minimum(jnp.maximum(result, -limit), limit).astype(held_as)


def setup_inputs(seed: int = 0) -> dict:
    arg_keys = jax.random.split(jax.random.key(seed), 7)
    tokens = noise(arg_keys[0], (TOKENS, D), 1.0, 6.0, ((0, 64),))
    expert_ids_keys = jax.random.split(jax.random.fold_in(arg_keys[1], 1), TOKENS // TOK_DEV)
    expert_ids_turns = jax.random.permutation(jax.random.fold_in(arg_keys[1], 3), TOKENS // TOK_DEV)
    expert_ids = jax.vmap(lambda own, number: routed_block(jax.random.fold_in(arg_keys[1], 2), own, number, TOK_DEV, EXPERTS, TOP, MOST, 2))(expert_ids_keys, expert_ids_turns).reshape((TOKENS, TOP))
    route_weight = jnp.clip(0.1 + 0.5 * jax.random.uniform(arg_keys[2], (TOKENS, TOP), jnp.float32) ** shard_levels(arg_keys[2], (TOKENS, TOP), ((0, 64),), -0.2, 0.2), 0.1, 0.6)
    gate_weight = noise(arg_keys[3], (EXPERTS, D, FF), D ** -0.5, 0.0625, ((0, 32), (2, 12)))
    up_weight = noise(arg_keys[4], (EXPERTS, D, FF), D ** -0.5, 0.0625, ((0, 32), (2, 12)))
    down_weight = noise(arg_keys[5], (EXPERTS, FF, D), FF ** -0.5, 0.15625, ((0, 32), (1, 12)))
    return {"tokens": tokens, "expert_ids": expert_ids, "route_weight": route_weight, "gate_weight": gate_weight, "up_weight": up_weight, "down_weight": down_weight}


def run_expert(packed):
    row_data, gate_w, up_w, down_w = packed
    gate_proj = jnp.dot(row_data, gate_w, preferred_element_type=jnp.float32)
    up_proj = jnp.dot(row_data, up_w, preferred_element_type=jnp.float32)
    hidden = (jax.nn.silu(gate_proj) * up_proj).astype(jnp.bfloat16)
    groups = hidden.reshape(hidden.shape[0], N_TP, FF // N_TP).astype(jnp.float32)
    pieces = down_w.reshape(N_TP, FF // N_TP, D).astype(jnp.float32)
    partial_sums = jnp.einsum("cgf,gfd->gcd", groups, pieces)
    return jnp.sum(partial_sums, 0)


def reference(tokens, expert_ids, route_weight, gate_weight, up_weight, down_weight):
    blocks = TOKENS // TOK_DEV
    chosen = expert_ids.reshape(blocks, TOK_DEV * TOP).astype(jnp.int32)
    onehot = (chosen[:, :, None] == jnp.arange(EXPERTS, dtype=jnp.int32)[None, None, :]).astype(jnp.int32)
    earlier = jnp.cumsum(onehot, 1) - onehot
    slot_index = jnp.sum(earlier * onehot, 2).astype(jnp.int32)
    position = (jnp.arange(blocks, dtype=jnp.int32)[:, None] * MOST + slot_index).reshape(-1).astype(jnp.int32)
    chosen_all = chosen.reshape(-1)
    token_index = (jnp.arange(TOKENS * TOP, dtype=jnp.int32) // TOP).astype(jnp.int32)
    capacity = blocks * MOST
    row_table = jnp.full((EXPERTS, capacity), TOKENS, jnp.int32).at[chosen_all, position].set(token_index)
    padded = jnp.concatenate([tokens, jnp.zeros((1, D), jnp.bfloat16)], 0)
    gathered_in = padded[row_table]
    expert_out = lax.map(run_expert, (gathered_in, gate_weight, up_weight, down_weight))
    picked = expert_out[chosen_all, position].reshape(TOKENS, TOP, D)
    mixed = jnp.sum(route_weight[:, :, None] * picked, 1)
    return mixed.astype(jnp.bfloat16)
```

```python
import jax
import jax.numpy as jnp
from jax import lax
from jax.sharding import PartitionSpec as P

TOP = 8
EXPERTS = 32
MOST = 8
LANES = 128
PARTS = 3


def ring(step):
    size = lax.axis_size("tp")
    return [(i, (i + step) % size) for i in range(size)]


def piece_width(width):
    tiles = -(-width // LANES)
    return -(-tiles // PARTS) * LANES


def piece_start(index, width):
    piece = piece_width(width)
    return jnp.minimum(lax.rem(index, PARTS) * piece, width - piece)


def positions(expert_ids):
    chosen = expert_ids.reshape(-1)
    onehot = (chosen[:, None] == jnp.arange(EXPERTS, dtype=jnp.int32)[None, :]).astype(jnp.int32)
    earlier = jnp.cumsum(onehot, 0) - onehot
    slot_index = jnp.sum(earlier * onehot, 1)
    position = chosen * MOST + slot_index
    return position.reshape(expert_ids.shape)


def gate_up_piece(gate_weight, up_weight, index):
    width = gate_weight.shape[1]
    start, piece = piece_start(index, width), piece_width(width)
    gate = lax.dynamic_slice_in_dim(gate_weight[0], start, piece, 0)
    up = lax.dynamic_slice_in_dim(up_weight[0], start, piece, 0)
    return jnp.concatenate([gate, up], 1)


def down_piece(down_weight, index):
    width = down_weight.shape[2]
    return lax.dynamic_slice_in_dim(
        down_weight[0], piece_start(index, width), piece_width(width), 1
    )


def combine(weight_table, returned):
    high = lax.reduce_precision(weight_table, 8, 7)
    low = weight_table - high
    both = jnp.concatenate([high, low], 0).astype(jnp.bfloat16)
    sums = jnp.dot(both, returned, preferred_element_type=jnp.float32)
    rows = weight_table.shape[0]
    return sums[:rows] + sums[rows:]


def per_device(tokens, expert_ids, route_weight, gate_weight, up_weight, down_weight):
    rows_here, width = tokens.shape
    capacity = EXPERTS * MOST
    piece = piece_width(width)
    tp_size = lax.axis_size("tp")
    here = lax.axis_index("tp")
    right = lax.rem(here + 1, tp_size)
    left = lax.rem(here + tp_size - 1, tp_size)

    gate_up_left = lax.ppermute(gate_up_piece(gate_weight, up_weight, right), "tp", ring(1))
    gate_up_right = lax.ppermute(gate_up_piece(gate_weight, up_weight, left), "tp", ring(-1))
    down_left = lax.ppermute(down_piece(down_weight, right), "tp", ring(1))
    down_right = lax.ppermute(down_piece(down_weight, left), "tp", ring(-1))

    position = positions(expert_ids)
    matches = position[:, :, None] == jnp.arange(capacity, dtype=jnp.int32)[None, None, :]
    dispatch = jnp.any(matches, 1).astype(jnp.bfloat16)
    weight_table = jnp.sum(jnp.where(matches, route_weight[:, :, None], 0.0), 1)

    start = piece_start(here, width)
    source = lax.dynamic_slice_in_dim(tokens, start, piece, 1)
    column = lax.broadcasted_iota(jnp.int32, source.shape, 1) + start
    source = jnp.where(column >= lax.rem(here, PARTS) * piece, source, jnp.zeros_like(source))
    outgoing = jnp.einsum(
        "tp,td->pd", dispatch, source, preferred_element_type=jnp.float32
    ).astype(jnp.bfloat16)
    outgoing = outgoing.reshape(EXPERTS, MOST, piece)
    received = lax.all_to_all(outgoing, "ep", split_axis=0, concat_axis=0, tiled=True)
    received = received.reshape(capacity, piece)

    def product(weights):
        return jnp.dot(received, weights, preferred_element_type=jnp.float32)

    from_right = lax.ppermute(product(gate_up_left), "tp", ring(-1))
    from_left = lax.ppermute(product(gate_up_right), "tp", ring(1))
    gate_up = product(gate_up_piece(gate_weight, up_weight, here)) + from_right + from_left
    units = gate_weight.shape[2]
    hidden = (jax.nn.silu(gate_up[:, :units]) * gate_up[:, units:]).astype(jnp.bfloat16)
    hidden_left = lax.ppermute(hidden, "tp", ring(1))
    hidden_right = lax.ppermute(hidden, "tp", ring(-1))

    partial_rows = jnp.dot(
        jnp.concatenate([hidden_left, hidden, hidden_right], 1),
        jnp.concatenate([down_left, down_piece(down_weight, here), down_right], 0),
        preferred_element_type=jnp.float32,
    ).astype(jnp.bfloat16)
    partial_rows = partial_rows.reshape(EXPERTS, MOST, piece)
    returned = lax.all_to_all(partial_rows, "ep", split_axis=0, concat_axis=0, tiled=True)
    combined = combine(weight_table, returned.reshape(capacity, piece))

    pieces = combined.reshape(tp_size, rows_here // tp_size, piece)
    arrived = lax.all_to_all(pieces, "tp", split_axis=0, concat_axis=0, tiled=True)
    arrived = arrived.reshape(tp_size // PARTS, PARTS, rows_here // tp_size, piece).sum(0)
    skip = PARTS * piece - width
    parts = [arrived[i] for i in range(PARTS)]
    parts[-1] = parts[-1][:, skip:]
    return jnp.concatenate(parts, 1).astype(jnp.bfloat16)


def solution(mesh):
    in_specs = (
        P(("ep", "dp"), None),
        P(("ep", "dp"), None),
        P(("ep", "dp"), None),
        P("ep", None, "tp"),
        P("ep", None, "tp"),
        P("ep", "tp", None),
    )
    out_specs = P(("ep", "dp", "tp"), None)
    return jax.shard_map(
        per_device, mesh=mesh, in_specs=in_specs, out_specs=out_specs, check_vma=False
    )
```

```python
import jax
import jax.numpy as jnp
from jax import lax
from jax.sharding import PartitionSpec as P

TOP = 8
EXPERTS = 32
MOST = 8
LANES = 128
PARTS = 3
CHUNKS = 2


def shift(array, step):
    size = lax.axis_size("tp")
    pairs = [
        (core * size + i, core * size + (i + sign * step) % size)
        for core, sign in ((0, 1), (1, -1))
        for i in range(size)
    ]
    return lax.ppermute(array, ("dp", "tp"), pairs)


def swap(array):
    return lax.ppermute(array, "dp", [(0, 1), (1, 0)])


def piece_width(width):
    tiles = -(-width // LANES)
    return -(-tiles // PARTS) * LANES


def piece_start(index, width):
    piece = piece_width(width)
    return jnp.minimum(lax.rem(index, PARTS) * piece, width - piece)


def positions(expert_ids):
    chosen = expert_ids.reshape(-1)
    onehot = (chosen[:, None] == jnp.arange(EXPERTS, dtype=jnp.int32)[None, :]).astype(jnp.int32)
    earlier = jnp.cumsum(onehot, 0) - onehot
    slot_index = jnp.sum(earlier * onehot, 1)
    slots = MOST // CHUNKS
    chunk = slot_index // slots
    position = chunk * EXPERTS * slots + chosen * slots + slot_index % slots
    return position.reshape(expert_ids.shape)


def gate_up_piece(gate_weight, up_weight, index):
    width = gate_weight.shape[1]
    start, piece = piece_start(index, width), piece_width(width)
    gate = lax.dynamic_slice_in_dim(gate_weight[0], start, piece, 0)
    up = lax.dynamic_slice_in_dim(up_weight[0], start, piece, 0)
    return jnp.concatenate([gate, up], 1)


def down_piece(down_weight, index):
    width = down_weight.shape[2]
    return lax.dynamic_slice_in_dim(
        down_weight[0], piece_start(index, width), piece_width(width), 1
    )


def combine(weight_table, returned):
    high = lax.reduce_precision(weight_table, 8, 7)
    low = weight_table - high
    both = jnp.concatenate([high, low], 0).astype(jnp.bfloat16)
    sums = jnp.dot(both, returned, preferred_element_type=jnp.float32)
    rows = weight_table.shape[0]
    return sums[:rows] + sums[rows:]


def per_device(tokens, expert_ids, route_weight, gate_weight, up_weight, down_weight):
    rows_here, width = tokens.shape
    piece = piece_width(width)
    tp_size = lax.axis_size("tp")
    here = lax.axis_index("tp")
    target = lax.rem(here + jnp.where(lax.axis_index("dp") == 0, 1, tp_size - 1), tp_size)

    gate_up_near = shift(gate_up_piece(gate_weight, up_weight, target), 1)
    gate_up_far = swap(gate_up_near)
    down_near = shift(down_piece(down_weight, target), 1)
    down_far = swap(down_near)
    gate_up_here = gate_up_piece(gate_weight, up_weight, here)
    down_all = jnp.concatenate([down_near, down_piece(down_weight, here), down_far], 0)
    units = gate_weight.shape[2]

    position = positions(expert_ids)
    matches = position[:, :, None] == jnp.arange(EXPERTS * MOST, dtype=jnp.int32)[None, None, :]
    dispatch = jnp.any(matches, 1).astype(jnp.bfloat16)
    weight_table = jnp.sum(jnp.where(matches, route_weight[:, :, None], 0.0), 1)

    start = piece_start(here, width)
    source = lax.dynamic_slice_in_dim(tokens, start, piece, 1)
    column = lax.broadcasted_iota(jnp.int32, source.shape, 1) + start
    source = jnp.where(column >= lax.rem(here, PARTS) * piece, source, jnp.zeros_like(source))

    slots = MOST // CHUNKS
    rows = EXPERTS * slots
    combined = 0.0
    for chunk in range(CHUNKS):
        span = slice(chunk * rows, (chunk + 1) * rows)
        outgoing = jnp.einsum(
            "tp,td->pd", dispatch[:, span], source, preferred_element_type=jnp.float32
        ).astype(jnp.bfloat16)
        outgoing = outgoing.reshape(EXPERTS, slots, piece)
        received = lax.all_to_all(outgoing, "ep", split_axis=0, concat_axis=0, tiled=True)
        received = received.reshape(rows, piece)

        def product(weights):
            return jnp.dot(received, weights, preferred_element_type=jnp.float32)

        from_far = shift(product(gate_up_near), -1)
        from_near = shift(product(gate_up_far), 1)
        gate_up = product(gate_up_here) + from_far + from_near
        hidden = (jax.nn.silu(gate_up[:, :units]) * gate_up[:, units:]).astype(jnp.bfloat16)
        hidden_near, hidden_far = shift(hidden, 1), shift(hidden, -1)
        partial_rows = jnp.dot(
            jnp.concatenate([hidden_near, hidden, hidden_far], 1),
            down_all,
            preferred_element_type=jnp.float32,
        ).astype(jnp.bfloat16)
        partial_rows = partial_rows.reshape(EXPERTS, slots, piece)
        returned = lax.all_to_all(partial_rows, "ep", split_axis=0, concat_axis=0, tiled=True)
        combined += combine(weight_table[:, span], returned.reshape(rows, piece))

    pieces = combined.reshape(tp_size, rows_here // tp_size, piece)
    arrived = lax.all_to_all(pieces, "tp", split_axis=0, concat_axis=0, tiled=True)
    arrived = arrived.reshape(tp_size // PARTS, PARTS, rows_here // tp_size, piece).sum(0)
    skip = PARTS * piece - width
    parts = [arrived[i] for i in range(PARTS)]
    parts[-1] = parts[-1][:, skip:]
    return jnp.concatenate(parts, 1).astype(jnp.bfloat16)


def solution(mesh):
    in_specs = (
        P(("ep", "dp"), None),
        P(("ep", "dp"), None),
        P(("ep", "dp"), None),
        P("ep", None, "tp"),
        P("ep", None, "tp"),
        P("ep", "tp", None),
    )
    out_specs = P(("ep", "dp", "tp"), None)
    return jax.shard_map(
        per_device, mesh=mesh, in_specs=in_specs, out_specs=out_specs, check_vma=False
    )
```

```python
import jax
import jax.numpy as jnp
from jax import lax
from jax.sharding import PartitionSpec as P

EXPERTS = 32
MOST = 8
LANES = 128
PARTS = 3


def shift(array, step):
    size = lax.axis_size("tp")
    pairs = [
        (core * size + i, core * size + (i + sign * step) % size)
        for core, sign in ((0, 1), (1, -1))
        for i in range(size)
    ]
    return lax.ppermute(array, ("dp", "tp"), pairs)


def swap(array):
    return lax.ppermute(array, "dp", [(0, 1), (1, 0)])


def exchange(array, axis):
    return lax.all_to_all(array, axis, split_axis=0, concat_axis=0, tiled=True)


def piece_width(width):
    tiles = -(-width // LANES)
    return -(-tiles // PARTS) * LANES


def piece_start(index, width):
    piece = piece_width(width)
    return jnp.minimum(lax.rem(index, PARTS) * piece, width - piece)


def positions(expert_ids):
    chosen = expert_ids.reshape(-1)
    onehot = (chosen[:, None] == jnp.arange(EXPERTS, dtype=jnp.int32)[None, :]).astype(jnp.int32)
    earlier = jnp.cumsum(onehot, 0) - onehot
    slot_index = jnp.sum(earlier * onehot, 1)
    position = chosen * MOST + slot_index
    return position.reshape(expert_ids.shape)


def gate_up_piece(gate_weight, up_weight, index):
    width = gate_weight.shape[1]
    start, piece = piece_start(index, width), piece_width(width)
    gate = lax.dynamic_slice_in_dim(gate_weight[0], start, piece, 0)
    up = lax.dynamic_slice_in_dim(up_weight[0], start, piece, 0)
    return jnp.concatenate([gate, up], 1)


def down_piece(down_weight, index):
    width = down_weight.shape[2]
    return lax.dynamic_slice_in_dim(
        down_weight[0], piece_start(index, width), piece_width(width), 1
    )


def combine(weight_table, returned):
    high = lax.reduce_precision(weight_table, 8, 7)
    low = weight_table - high
    both = jnp.concatenate([high, low], 0).astype(jnp.bfloat16)
    sums = jnp.dot(both, returned, preferred_element_type=jnp.float32)
    rows = weight_table.shape[0]
    return sums[:rows] + sums[rows:]


def per_device(tokens, expert_ids, route_weight, gate_weight, up_weight, down_weight):
    rows_here, width = tokens.shape
    piece = piece_width(width)
    units = gate_weight.shape[2]
    capacity = EXPERTS * MOST
    tp_size = lax.axis_size("tp")
    here = lax.axis_index("tp")
    target = lax.rem(here + jnp.where(lax.axis_index("dp") == 0, 1, tp_size - 1), tp_size)

    sent = gate_up_piece(gate_weight, up_weight, target)
    sent, expert_ids, tokens = lax.optimization_barrier((sent, expert_ids, tokens))
    gate_up_near = shift(sent, 1)
    gate_up_far = swap(gate_up_near)

    position = positions(expert_ids)
    matches = position[:, :, None] == jnp.arange(capacity, dtype=jnp.int32)[None, None, :]
    dispatch = jnp.any(matches, 1).astype(jnp.bfloat16)

    start = piece_start(here, width)
    source = lax.dynamic_slice_in_dim(tokens, start, piece, 1)
    column = lax.broadcasted_iota(jnp.int32, source.shape, 1) + start
    source = jnp.where(column >= lax.rem(here, PARTS) * piece, source, jnp.zeros_like(source))
    outgoing = jnp.einsum(
        "tp,td->pd", dispatch, source, preferred_element_type=jnp.float32
    ).astype(jnp.bfloat16)
    outgoing, gate_weight, up_weight, down_weight = lax.optimization_barrier(
        (outgoing, gate_weight, up_weight, down_weight)
    )
    received = exchange(outgoing.reshape(EXPERTS, MOST, piece), "ep")
    received = received.reshape(capacity, piece)

    down_near = shift(down_piece(down_weight, target), 1)
    down_far = swap(down_near)

    def product(weights):
        return jnp.dot(received, weights, preferred_element_type=jnp.float32)

    from_far = shift(product(gate_up_near).astype(jnp.bfloat16), -1)
    from_near = shift(product(gate_up_far).astype(jnp.bfloat16), 1)
    gate_up = product(gate_up_piece(gate_weight, up_weight, here))
    gate_up = gate_up + from_far.astype(jnp.float32) + from_near.astype(jnp.float32)
    hidden = (jax.nn.silu(gate_up[:, :units]) * gate_up[:, units:]).astype(jnp.bfloat16)
    hidden_near, hidden_far = shift(hidden, 1), shift(hidden, -1)
    partial_rows = jnp.dot(
        jnp.concatenate([hidden_near, hidden, hidden_far], 1),
        jnp.concatenate([down_near, down_piece(down_weight, here), down_far], 0),
        preferred_element_type=jnp.float32,
    ).astype(jnp.bfloat16)
    returned = exchange(partial_rows.reshape(EXPERTS, MOST, piece), "ep")
    weight_table = jnp.sum(jnp.where(matches, route_weight[:, :, None], 0.0), 1)
    combined = combine(weight_table, returned.reshape(capacity, piece)).astype(jnp.bfloat16)

    pieces = combined.reshape(tp_size, rows_here // tp_size, piece)
    arrived = exchange(pieces, "tp")
    arrived = arrived.reshape(tp_size // PARTS, PARTS, rows_here // tp_size, piece)
    arrived = sum(arrived[i].astype(jnp.float32) for i in range(tp_size // PARTS))
    skip = PARTS * piece - width
    parts = [arrived[i] for i in range(PARTS)]
    parts[-1] = parts[-1][:, skip:]
    return jnp.concatenate(parts, 1).astype(jnp.bfloat16)


def solution(mesh):
    in_specs = (
        P(("ep", "dp"), None),
        P(("ep", "dp"), None),
        P(("ep", "dp"), None),
        P("ep", None, "tp"),
        P("ep", None, "tp"),
        P("ep", "tp", None),
    )
    out_specs = P(("ep", "dp", "tp"), None)
    return jax.shard_map(
        per_device, mesh=mesh, in_specs=in_specs, out_specs=out_specs, check_vma=False
    )
```

```python
import jax
import jax.numpy as jnp
from jax import lax
from jax.experimental import pallas as pl
from jax.experimental.pallas import tpu as pltpu
from jax.sharding import PartitionSpec as P

TOP = 8
EXPERTS = 32
MOST = 8
LANES = 128
PARTS = 3


def shift(array, step):
    size = lax.axis_size("tp")
    pairs = [
        (core * size + i, core * size + (i + sign * step) % size)
        for core, sign in ((0, 1), (1, -1))
        for i in range(size)
    ]
    return lax.ppermute(array, ("dp", "tp"), pairs)


def swap(array):
    return lax.ppermute(array, "dp", [(0, 1), (1, 0)])


def exchange(array, axis):
    return lax.all_to_all(array, axis, split_axis=0, concat_axis=0, tiled=True)


def piece_width(width):
    tiles = -(-width // LANES)
    return -(-tiles // PARTS) * LANES


def piece_start(index, width):
    piece = piece_width(width)
    return jnp.minimum(lax.rem(index, PARTS) * piece, width - piece)


def cut_gate_up(start_ref, gate_ref, up_ref, out_ref, sem):
    piece, units = out_ref.shape[0], gate_ref.shape[2]
    rows = pl.ds(pl.multiple_of(start_ref[0], LANES), piece)
    copies = [
        pltpu.make_async_copy(
            ref.at[0, rows, :], out_ref.at[:, pl.ds(i * units, units)], sem.at[i]
        )
        for i, ref in enumerate((gate_ref, up_ref))
    ]
    for copy in copies:
        copy.start()
    for copy in copies:
        copy.wait()


def cut_down(start_ref, down_ref, out_ref, sem):
    columns = pl.ds(pl.multiple_of(start_ref[0], LANES), out_ref.shape[1])
    copy = pltpu.make_async_copy(down_ref.at[0, :, columns], out_ref, sem.at[0])
    copy.start()
    copy.wait()


def cut(kernel, start, arrays, shape):
    size = shape[0] * shape[1]
    return pl.pallas_call(
        kernel,
        out_shape=jax.ShapeDtypeStruct(shape, jnp.bfloat16),
        in_specs=[pl.BlockSpec(memory_space=pltpu.SMEM)]
        + [pl.BlockSpec(memory_space=pl.ANY)] * len(arrays),
        out_specs=pl.BlockSpec(memory_space=pltpu.VMEM),
        scratch_shapes=[pltpu.SemaphoreType.DMA((2,))],
        cost_estimate=pl.CostEstimate(
            flops=500 * size, bytes_accessed=4 * size, transcendentals=0
        ),
    )(start.reshape(1), *arrays)


def gate_up_piece(gate_weight, up_weight, index):
    width, units = gate_weight.shape[1:]
    shape = (piece_width(width), 2 * units)
    return cut(cut_gate_up, piece_start(index, width), (gate_weight, up_weight), shape)


def down_piece(down_weight, index):
    units, width = down_weight.shape[1:]
    shape = (units, piece_width(width))
    return cut(cut_down, piece_start(index, width), (down_weight,), shape)


def dispatch_kernel(where_ref, ids_ref, route_ref, tokens_ref, rows_ref, weights_ref, held, sem):
    tokens, piece = held.shape
    capacity = rows_ref.shape[0]
    start = pl.multiple_of(where_ref[0], LANES)
    copy = pltpu.make_async_copy(tokens_ref.at[:, pl.ds(start, piece)], held, sem.at[0])
    copy.start()
    lane = lax.broadcasted_iota(jnp.int32, (tokens, capacity), 1)
    expert, slot = lane // MOST, lane % MOST
    member = jnp.zeros((tokens, capacity), jnp.float32)
    weight = jnp.zeros((tokens, capacity), jnp.float32)
    for k in range(TOP):
        same = ids_ref[:, k : k + 1] == expert
        member = jnp.where(same, 1.0, member)
        weight = jnp.where(same, route_ref[:, k : k + 1], weight)
    row = lax.broadcasted_iota(jnp.int32, (tokens, tokens), 0)
    column = lax.broadcasted_iota(jnp.int32, (tokens, tokens), 1)
    above = jnp.where(column < row, 1.0, 0.0).astype(jnp.bfloat16)
    earlier = jnp.dot(above, member.astype(jnp.bfloat16), preferred_element_type=jnp.float32)
    here = earlier == slot.astype(jnp.float32)
    chosen = jnp.where(here, member, 0.0).astype(jnp.bfloat16)
    weight = jnp.where(here, weight, 0.0)
    high = weight.astype(jnp.bfloat16)
    weights_ref[0] = high
    weights_ref[1] = (weight - high.astype(jnp.float32)).astype(jnp.bfloat16)
    copy.wait()
    wide = lax.broadcasted_iota(jnp.int32, (tokens, piece), 1)
    source = jnp.where(wide >= where_ref[1], held[...].astype(jnp.float32), 0.0)
    rows_ref[...] = lax.dot_general(
        chosen,
        source.astype(jnp.bfloat16),
        (((0,), (0,)), ((), ())),
        preferred_element_type=jnp.float32,
    ).astype(jnp.bfloat16)


def dispatch(tokens, expert_ids, route_weight, index):
    count, width = tokens.shape
    piece, capacity = piece_width(width), EXPERTS * MOST
    start = piece_start(index, width)
    where = jnp.stack([start, lax.rem(index, PARTS) * piece - start])
    return pl.pallas_call(
        dispatch_kernel,
        out_shape=(
            jax.ShapeDtypeStruct((capacity, piece), jnp.bfloat16),
            jax.ShapeDtypeStruct((2, count, capacity), jnp.bfloat16),
        ),
        in_specs=[pl.BlockSpec(memory_space=pltpu.SMEM)]
        + [pl.BlockSpec(memory_space=pltpu.VMEM)] * 2
        + [pl.BlockSpec(memory_space=pl.ANY)],
        out_specs=(pl.BlockSpec(memory_space=pltpu.VMEM),) * 2,
        scratch_shapes=[pltpu.VMEM((count, piece), jnp.bfloat16), pltpu.SemaphoreType.DMA((1,))],
        cost_estimate=pl.CostEstimate(
            flops=2 * count * piece * capacity, bytes_accessed=2**21, transcendentals=0
        ),
        name="dispatch",
    )(where, expert_ids, route_weight, tokens)


def combine(weights, returned):
    parts, rows, capacity = weights.shape
    both = weights.reshape(parts * rows, capacity)
    sums = jnp.dot(both, returned, preferred_element_type=jnp.float32)
    return sums[:rows] + sums[rows:]


def per_device(tokens, expert_ids, route_weight, gate_weight, up_weight, down_weight):
    rows_here, width = tokens.shape
    piece = piece_width(width)
    units = gate_weight.shape[2]
    capacity = EXPERTS * MOST
    tp_size = lax.axis_size("tp")
    here = lax.axis_index("tp")
    target = lax.rem(here + jnp.where(lax.axis_index("dp") == 0, 1, tp_size - 1), tp_size)

    outgoing, weights = dispatch(tokens, expert_ids, route_weight, here)
    outgoing, gate_weight, up_weight, down_weight = lax.optimization_barrier(
        (outgoing, gate_weight, up_weight, down_weight)
    )
    received = exchange(outgoing.reshape(EXPERTS, MOST, piece), "ep")
    received = received.reshape(capacity, piece)

    gate_up_near = shift(gate_up_piece(gate_weight, up_weight, target), 1)
    gate_up_far = swap(gate_up_near)
    down_near = shift(down_piece(down_weight, target), 1)
    down_far = swap(down_near)
    gate_weight, up_weight, down_weight, _ = lax.optimization_barrier(
        (gate_weight, up_weight, down_weight, gate_up_near)
    )
    gate_up_here = gate_up_piece(gate_weight, up_weight, here)
    down_here = down_piece(down_weight, here)

    def product(weights):
        return jnp.dot(received, weights, preferred_element_type=jnp.float32)

    from_far = shift(product(gate_up_near).astype(jnp.bfloat16), -1)
    from_near = shift(product(gate_up_far).astype(jnp.bfloat16), 1)
    gate_up = product(gate_up_here)
    gate_up = gate_up + from_far.astype(jnp.float32) + from_near.astype(jnp.float32)
    hidden = (jax.nn.silu(gate_up[:, :units]) * gate_up[:, units:]).astype(jnp.bfloat16)
    hidden_near, hidden_far = shift(hidden, 1), shift(hidden, -1)
    partial_rows = jnp.dot(
        jnp.concatenate([hidden_near, hidden, hidden_far], 1),
        jnp.concatenate([down_near, down_here, down_far], 0),
        preferred_element_type=jnp.float32,
    ).astype(jnp.bfloat16)
    returned = exchange(partial_rows.reshape(EXPERTS, MOST, piece), "ep")
    combined = combine(weights, returned.reshape(capacity, piece)).astype(jnp.bfloat16)

    pieces = combined.reshape(tp_size, rows_here // tp_size, piece)
    arrived = exchange(pieces, "tp")
    arrived = arrived.reshape(tp_size // PARTS, PARTS, rows_here // tp_size, piece)
    arrived = sum(arrived[i].astype(jnp.float32) for i in range(tp_size // PARTS))
    skip = PARTS * piece - width
    parts = [arrived[i] for i in range(PARTS)]
    parts[-1] = parts[-1][:, skip:]
    return jnp.concatenate(parts, 1).astype(jnp.bfloat16)


def solution(mesh):
    in_specs = (
        P(("ep", "dp"), None),
        P(("ep", "dp"), None),
        P(("ep", "dp"), None),
        P("ep", None, "tp"),
        P("ep", None, "tp"),
        P("ep", "tp", None),
    )
    out_specs = P(("ep", "dp", "tp"), None)
    return jax.shard_map(
        per_device, mesh=mesh, in_specs=in_specs, out_specs=out_specs, check_vma=False
    )
```

```python
import jax
import jax.numpy as jnp
from jax import lax
from jax.experimental import pallas as pl
from jax.experimental.pallas import tpu as pltpu
from jax.sharding import PartitionSpec as P

TOP = 8
EXPERTS = 32
MOST = 8
LANES = 128
PARTS = 3
BLOCK = 5 * LANES


def shift(array, step):
    size = lax.axis_size("tp")
    pairs = [
        (core * size + i, core * size + (i + sign * step) % size)
        for core, sign in ((0, 1), (1, -1))
        for i in range(size)
    ]
    return lax.ppermute(array, ("dp", "tp"), pairs)


def swap(array):
    return lax.ppermute(array, "dp", [(0, 1), (1, 0)])


def exchange(array, axis):
    return lax.all_to_all(array, axis, split_axis=0, concat_axis=0, tiled=True)


def piece_width(width):
    tiles = -(-width // LANES)
    return -(-tiles // PARTS) * LANES


def piece_start(index, width):
    piece = piece_width(width)
    return jnp.minimum(lax.rem(index, PARTS) * piece, width - piece)


def cut_gate_up(start_ref, gate_ref, up_ref, out_ref, sem):
    piece, units = out_ref.shape[0], gate_ref.shape[2]
    rows = pl.ds(pl.multiple_of(start_ref[0], LANES), piece)
    copies = [
        pltpu.make_async_copy(
            ref.at[0, rows, :], out_ref.at[:, pl.ds(i * units, units)], sem.at[i]
        )
        for i, ref in enumerate((gate_ref, up_ref))
    ]
    for copy in copies:
        copy.start()
    for copy in copies:
        copy.wait()


def cut_down(start_ref, down_ref, out_ref, sem):
    columns = pl.ds(pl.multiple_of(start_ref[0], LANES), out_ref.shape[1])
    copy = pltpu.make_async_copy(down_ref.at[0, :, columns], out_ref, sem.at[0])
    copy.start()
    copy.wait()


def cut(kernel, start, arrays, shape):
    size = shape[0] * shape[1]
    return pl.pallas_call(
        kernel,
        out_shape=jax.ShapeDtypeStruct(shape, jnp.bfloat16),
        in_specs=[pl.BlockSpec(memory_space=pltpu.SMEM)]
        + [pl.BlockSpec(memory_space=pl.ANY)] * len(arrays),
        out_specs=pl.BlockSpec(memory_space=pltpu.VMEM),
        scratch_shapes=[pltpu.SemaphoreType.DMA((2,))],
        cost_estimate=pl.CostEstimate(
            flops=500 * size, bytes_accessed=4 * size, transcendentals=0
        ),
    )(start.reshape(1), *arrays)


def gate_up_piece(gate_weight, up_weight, index):
    width, units = gate_weight.shape[1:]
    shape = (piece_width(width), 2 * units)
    return cut(cut_gate_up, piece_start(index, width), (gate_weight, up_weight), shape)


def down_piece(down_weight, index):
    units, width = down_weight.shape[1:]
    shape = (units, piece_width(width))
    return cut(cut_down, piece_start(index, width), (down_weight,), shape)


def dispatch_kernel(start_ref, ids_ref, tokens_ref, rows_ref, held, chosen, sem):
    capacity, count = chosen.shape
    width = tokens_ref.shape[1]
    piece = piece_width(width)
    block = rows_ref.shape[1]
    step = pl.program_id(0)

    @pl.when(step == 0)
    def _():
        start = pl.multiple_of(start_ref[0], LANES)
        copy = pltpu.make_async_copy(
            tokens_ref.at[:, pl.ds(start, piece)], held.at[:, pl.ds(0, piece)], sem.at[0]
        )
        copy.start()
        line = lax.broadcasted_iota(jnp.int32, (capacity, count), 0)
        expert, slot = line // MOST, line % MOST
        member = jnp.zeros((capacity, count), jnp.float32)
        for k in range(TOP):
            member = jnp.where(ids_ref[k : k + 1, :] == expert, 1.0, member)
        row = lax.broadcasted_iota(jnp.int32, (count, count), 0)
        column = lax.broadcasted_iota(jnp.int32, (count, count), 1)
        before = jnp.where(row < column, 1.0, 0.0).astype(jnp.bfloat16)
        earlier = jnp.dot(member.astype(jnp.bfloat16), before, preferred_element_type=jnp.float32)
        here = earlier == slot.astype(jnp.float32)
        chosen[...] = jnp.where(here, member, 0.0).astype(jnp.bfloat16)
        copy.wait()

    first = jnp.where(start_ref[0] == width - piece, PARTS * piece - width, 0)
    source = held[:, pl.ds(pl.multiple_of(step * block, LANES), block)]
    wide = lax.broadcasted_iota(jnp.int32, source.shape, 1) + step * block
    source = jnp.where(wide >= first, source.astype(jnp.float32), 0.0).astype(jnp.bfloat16)
    rows_ref[...] = jnp.dot(chosen[...], source, preferred_element_type=jnp.float32).astype(
        jnp.bfloat16
    )


def dispatch(tokens, expert_ids, index):
    count, width = tokens.shape
    piece, capacity = piece_width(width), EXPERTS * MOST
    steps = -(-piece // BLOCK)
    return pl.pallas_call(
        dispatch_kernel,
        grid=(steps,),
        out_shape=jax.ShapeDtypeStruct((capacity, piece), jnp.bfloat16),
        in_specs=[
            pl.BlockSpec(memory_space=pltpu.SMEM),
            pl.BlockSpec((TOP, count), lambda i: (0, 0)),
            pl.BlockSpec(memory_space=pl.ANY),
        ],
        out_specs=pl.BlockSpec((capacity, BLOCK), lambda i: (0, i)),
        scratch_shapes=[
            pltpu.VMEM((count, steps * BLOCK), jnp.bfloat16),
            pltpu.VMEM((capacity, count), jnp.bfloat16),
            pltpu.SemaphoreType.DMA((1,)),
        ],
        cost_estimate=pl.CostEstimate(
            flops=2 * count * piece * capacity, bytes_accessed=2**21, transcendentals=0
        ),
        name="dispatch",
    )(piece_start(index, width).reshape(1), expert_ids.T, tokens)


def weigh_kernel(ids_ref, route_ref, weights_ref):
    count, capacity = weights_ref.shape[1:]
    lane = lax.broadcasted_iota(jnp.int32, (count, capacity), 1)
    expert, slot = lane // MOST, lane % MOST
    member = jnp.zeros((count, capacity), jnp.float32)
    weight = jnp.zeros((count, capacity), jnp.float32)
    for k in range(TOP):
        same = ids_ref[:, k : k + 1] == expert
        member = jnp.where(same, 1.0, member)
        weight = jnp.where(same, route_ref[:, k : k + 1], weight)
    row = lax.broadcasted_iota(jnp.int32, (count, count), 0)
    column = lax.broadcasted_iota(jnp.int32, (count, count), 1)
    above = jnp.where(column < row, 1.0, 0.0).astype(jnp.bfloat16)
    earlier = jnp.dot(above, member.astype(jnp.bfloat16), preferred_element_type=jnp.float32)
    weight = jnp.where(earlier == slot.astype(jnp.float32), weight, 0.0)
    high = weight.astype(jnp.bfloat16)
    weights_ref[0] = high
    weights_ref[1] = (weight - high.astype(jnp.float32)).astype(jnp.bfloat16)


def weigh(expert_ids, route_weight):
    shape = (2, expert_ids.shape[0], EXPERTS * MOST)
    return pl.pallas_call(
        weigh_kernel,
        out_shape=jax.ShapeDtypeStruct(shape, jnp.bfloat16),
        cost_estimate=pl.CostEstimate(
            flops=2**26, bytes_accessed=2**15, transcendentals=0
        ),
        name="weigh",
    )(expert_ids, route_weight)


def combine(weights, returned):
    parts, rows, capacity = weights.shape
    both = weights.reshape(parts * rows, capacity)
    sums = jnp.dot(both, returned, preferred_element_type=jnp.float32)
    return sums[:rows] + sums[rows:]


def per_device(tokens, expert_ids, route_weight, gate_weight, up_weight, down_weight):
    rows_here, width = tokens.shape
    piece = piece_width(width)
    units = gate_weight.shape[2]
    capacity = EXPERTS * MOST
    tp_size = lax.axis_size("tp")
    here = lax.axis_index("tp")
    target = lax.rem(here + jnp.where(lax.axis_index("dp") == 0, 1, tp_size - 1), tp_size)

    outgoing = dispatch(tokens, expert_ids, here)
    outgoing, gate_weight, up_weight, down_weight, expert_ids, route_weight = (
        lax.optimization_barrier(
            (outgoing, gate_weight, up_weight, down_weight, expert_ids, route_weight)
        )
    )
    received = exchange(outgoing.reshape(EXPERTS, MOST, piece), "ep")
    received = received.reshape(capacity, piece)

    gate_up_near = shift(gate_up_piece(gate_weight, up_weight, target), 1)
    gate_up_far = swap(gate_up_near)
    down_near = shift(down_piece(down_weight, target), 1)
    down_far = swap(down_near)
    gate_up_here = gate_up_piece(gate_weight, up_weight, here)
    down_here = down_piece(down_weight, here)
    weights = weigh(expert_ids, route_weight)

    def product(weights):
        return jnp.dot(received, weights, preferred_element_type=jnp.float32)

    from_far = shift(product(gate_up_near).astype(jnp.bfloat16), -1)
    from_near = shift(product(gate_up_far).astype(jnp.bfloat16), 1)
    gate_up = product(gate_up_here)
    gate_up = gate_up + from_far.astype(jnp.float32) + from_near.astype(jnp.float32)
    hidden = (jax.nn.silu(gate_up[:, :units]) * gate_up[:, units:]).astype(jnp.bfloat16)
    hidden_near, hidden_far = shift(hidden, 1), shift(hidden, -1)
    partial_rows = jnp.dot(
        jnp.concatenate([hidden_near, hidden, hidden_far], 1),
        jnp.concatenate([down_near, down_here, down_far], 0),
        preferred_element_type=jnp.float32,
    ).astype(jnp.bfloat16)
    returned = exchange(partial_rows.reshape(EXPERTS, MOST, piece), "ep")
    combined = combine(weights, returned.reshape(capacity, piece)).astype(jnp.bfloat16)

    pieces = combined.reshape(tp_size, rows_here // tp_size, piece)
    arrived = exchange(pieces, "tp")
    arrived = arrived.reshape(tp_size // PARTS, PARTS, rows_here // tp_size, piece)
    arrived = sum(arrived[i].astype(jnp.float32) for i in range(tp_size // PARTS))
    skip = PARTS * piece - width
    parts = [arrived[i] for i in range(PARTS)]
    parts[-1] = parts[-1][:, skip:]
    return jnp.concatenate(parts, 1).astype(jnp.bfloat16)


def solution(mesh):
    in_specs = (
        P(("ep", "dp"), None),
        P(("ep", "dp"), None),
        P(("ep", "dp"), None),
        P("ep", None, "tp"),
        P("ep", None, "tp"),
        P("ep", "tp", None),
    )
    out_specs = P(("ep", "dp", "tp"), None)
    return jax.shard_map(
        per_device, mesh=mesh, in_specs=in_specs, out_specs=out_specs, check_vma=False
    )
```

```python
import jax
import jax.numpy as jnp
from jax import lax
from jax.experimental import pallas as pl
from jax.experimental.pallas import tpu as pltpu
from jax.sharding import PartitionSpec as P

TOP = 8
EXPERTS = 32
MOST = 8
LANES = 128
PARTS = 3
BLOCK = 5 * LANES


def shift(array, step):
    size = lax.axis_size("tp")
    pairs = [
        (core * size + i, core * size + (i + sign * step) % size)
        for core, sign in ((0, 1), (1, -1))
        for i in range(size)
    ]
    return lax.ppermute(array, ("dp", "tp"), pairs)


def swap(array):
    return lax.ppermute(array, "dp", [(0, 1), (1, 0)])


def exchange(array, axis):
    return lax.all_to_all(array, axis, split_axis=0, concat_axis=0, tiled=True)


def piece_width(width):
    tiles = -(-width // LANES)
    return -(-tiles // PARTS) * LANES


def piece_start(index, width):
    piece = piece_width(width)
    return jnp.minimum(lax.rem(index, PARTS) * piece, width - piece)


def cut_gate_up(start_ref, gate_ref, up_ref, out_ref, sem):
    piece, units = out_ref.shape[0], gate_ref.shape[2]
    rows = pl.ds(pl.multiple_of(start_ref[0], LANES), piece)
    copies = [
        pltpu.make_async_copy(
            ref.at[0, rows, :], out_ref.at[:, pl.ds(i * units, units)], sem.at[i]
        )
        for i, ref in enumerate((gate_ref, up_ref))
    ]
    for copy in copies:
        copy.start()
    for copy in copies:
        copy.wait()


def cut_down(start_ref, down_ref, out_ref, sem):
    columns = pl.ds(pl.multiple_of(start_ref[0], LANES), out_ref.shape[1])
    copy = pltpu.make_async_copy(down_ref.at[0, :, columns], out_ref, sem.at[0])
    copy.start()
    copy.wait()


def cut(kernel, start, arrays, shape):
    size = shape[0] * shape[1]
    return pl.pallas_call(
        kernel,
        out_shape=jax.ShapeDtypeStruct(shape, jnp.bfloat16),
        in_specs=[pl.BlockSpec(memory_space=pltpu.SMEM)]
        + [pl.BlockSpec(memory_space=pl.ANY)] * len(arrays),
        out_specs=pl.BlockSpec(memory_space=pltpu.VMEM),
        scratch_shapes=[pltpu.SemaphoreType.DMA((2,))],
        cost_estimate=pl.CostEstimate(
            flops=500 * size, bytes_accessed=4 * size, transcendentals=0
        ),
    )(start.reshape(1), *arrays)


def gate_up_piece(gate_weight, up_weight, index):
    width, units = gate_weight.shape[1:]
    shape = (piece_width(width), 2 * units)
    return cut(cut_gate_up, piece_start(index, width), (gate_weight, up_weight), shape)


def down_piece(down_weight, index):
    units, width = down_weight.shape[1:]
    shape = (units, piece_width(width))
    return cut(cut_down, piece_start(index, width), (down_weight,), shape)


def dispatch_kernel(start_ref, ids_ref, tokens_ref, rows_ref, ids, held, chosen, sem):
    capacity, count = chosen.shape
    width = tokens_ref.shape[1]
    piece = piece_width(width)
    block = rows_ref.shape[1]
    step = pl.program_id(0)

    @pl.when(step == 0)
    def _():
        ids_copy = pltpu.make_async_copy(ids_ref, ids, sem.at[1])
        ids_copy.start()
        start = pl.multiple_of(start_ref[0], LANES)
        copy = pltpu.make_async_copy(
            tokens_ref.at[:, pl.ds(start, piece)], held.at[:, pl.ds(0, piece)], sem.at[0]
        )
        copy.start()
        line = lax.broadcasted_iota(jnp.int32, (capacity, count), 0)
        expert, slot = line // MOST, line % MOST
        member = jnp.zeros((capacity, count), jnp.float32)
        ids_copy.wait()
        for k in range(TOP):
            member = jnp.where(ids[k : k + 1, :] == expert, 1.0, member)
        row = lax.broadcasted_iota(jnp.int32, (count, count), 0)
        column = lax.broadcasted_iota(jnp.int32, (count, count), 1)
        before = jnp.where(row < column, 1.0, 0.0).astype(jnp.bfloat16)
        earlier = jnp.dot(member.astype(jnp.bfloat16), before, preferred_element_type=jnp.float32)
        here = earlier == slot.astype(jnp.float32)
        chosen[...] = jnp.where(here, member, 0.0).astype(jnp.bfloat16)
        copy.wait()

    first = jnp.where(start_ref[0] == width - piece, PARTS * piece - width, 0)
    source = held[:, pl.ds(pl.multiple_of(step * block, LANES), block)]
    wide = lax.broadcasted_iota(jnp.int32, source.shape, 1) + step * block
    source = jnp.where(wide >= first, source.astype(jnp.float32), 0.0).astype(jnp.bfloat16)
    rows_ref[...] = jnp.dot(chosen[...], source, preferred_element_type=jnp.float32).astype(
        jnp.bfloat16
    )


def dispatch(tokens, expert_ids, index):
    count, width = tokens.shape
    piece, capacity = piece_width(width), EXPERTS * MOST
    steps = -(-piece // BLOCK)
    return pl.pallas_call(
        dispatch_kernel,
        grid=(steps,),
        out_shape=jax.ShapeDtypeStruct((capacity, piece), jnp.bfloat16),
        in_specs=[
            pl.BlockSpec(memory_space=pltpu.SMEM),
            pl.BlockSpec(memory_space=pl.ANY),
            pl.BlockSpec(memory_space=pl.ANY),
        ],
        out_specs=pl.BlockSpec((capacity, BLOCK), lambda i: (0, i)),
        scratch_shapes=[
            pltpu.VMEM((TOP, count), jnp.int32),
            pltpu.VMEM((count, steps * BLOCK), jnp.bfloat16),
            pltpu.VMEM((capacity, count), jnp.bfloat16),
            pltpu.SemaphoreType.DMA((2,)),
        ],
        cost_estimate=pl.CostEstimate(
            flops=2 * count * piece * capacity, bytes_accessed=2**21, transcendentals=0
        ),
        name="dispatch",
    )(piece_start(index, width).reshape(1), expert_ids.T, tokens)


def weigh_kernel(ids_ref, route_ref, weights_ref):
    count, capacity = weights_ref.shape[1:]
    lane = lax.broadcasted_iota(jnp.int32, (count, capacity), 1)
    expert, slot = lane // MOST, lane % MOST
    member = jnp.zeros((count, capacity), jnp.float32)
    weight = jnp.zeros((count, capacity), jnp.float32)
    for k in range(TOP):
        same = ids_ref[:, k : k + 1] == expert
        member = jnp.where(same, 1.0, member)
        weight = jnp.where(same, route_ref[:, k : k + 1], weight)
    row = lax.broadcasted_iota(jnp.int32, (count, count), 0)
    column = lax.broadcasted_iota(jnp.int32, (count, count), 1)
    above = jnp.where(column < row, 1.0, 0.0).astype(jnp.bfloat16)
    earlier = jnp.dot(above, member.astype(jnp.bfloat16), preferred_element_type=jnp.float32)
    weight = jnp.where(earlier == slot.astype(jnp.float32), weight, 0.0)
    high = weight.astype(jnp.bfloat16)
    weights_ref[0] = high
    weights_ref[1] = (weight - high.astype(jnp.float32)).astype(jnp.bfloat16)


def weigh(expert_ids, route_weight):
    shape = (2, expert_ids.shape[0], EXPERTS * MOST)
    return pl.pallas_call(
        weigh_kernel,
        out_shape=jax.ShapeDtypeStruct(shape, jnp.bfloat16),
        cost_estimate=pl.CostEstimate(
            flops=2**26, bytes_accessed=2**15, transcendentals=0
        ),
        name="weigh",
    )(expert_ids, route_weight)


def combine(weights, returned):
    parts, rows, capacity = weights.shape
    both = weights.reshape(parts * rows, capacity)
    sums = jnp.dot(both, returned, preferred_element_type=jnp.float32)
    return sums[:rows] + sums[rows:]


def per_device(tokens, expert_ids, route_weight, gate_weight, up_weight, down_weight):
    rows_here, width = tokens.shape
    piece = piece_width(width)
    units = gate_weight.shape[2]
    capacity = EXPERTS * MOST
    tp_size = lax.axis_size("tp")
    here = lax.axis_index("tp")
    target = lax.rem(here + jnp.where(lax.axis_index("dp") == 0, 1, tp_size - 1), tp_size)

    outgoing = dispatch(tokens, expert_ids, here)
    outgoing, gate_weight, up_weight, down_weight, expert_ids, route_weight = (
        lax.optimization_barrier(
            (outgoing, gate_weight, up_weight, down_weight, expert_ids, route_weight)
        )
    )
    received = exchange(outgoing.reshape(EXPERTS, MOST, piece), "ep")
    received = received.reshape(capacity, piece)

    gate_up_near = shift(gate_up_piece(gate_weight, up_weight, target), 1)
    gate_up_far = swap(gate_up_near)
    down_near = shift(down_piece(down_weight, target), 1)
    down_far = swap(down_near)
    gate_up_here = gate_up_piece(gate_weight, up_weight, here)
    down_here = down_piece(down_weight, here)
    weights = weigh(expert_ids, route_weight)

    def product(weights):
        return jnp.dot(received, weights, preferred_element_type=jnp.float32)

    from_far = shift(product(gate_up_near).astype(jnp.bfloat16), -1)
    from_near = shift(product(gate_up_far).astype(jnp.bfloat16), 1)
    gate_up = product(gate_up_here)
    gate_up = gate_up + from_far.astype(jnp.float32) + from_near.astype(jnp.float32)
    hidden = (jax.nn.silu(gate_up[:, :units]) * gate_up[:, units:]).astype(jnp.bfloat16)
    hidden_near, hidden_far = shift(hidden, 1), shift(hidden, -1)
    partial_rows = jnp.dot(
        jnp.concatenate([hidden_near, hidden, hidden_far], 1),
        jnp.concatenate([down_near, down_here, down_far], 0),
        preferred_element_type=jnp.float32,
    ).astype(jnp.bfloat16)
    returned = exchange(partial_rows.reshape(EXPERTS, MOST, piece), "ep")
    combined = combine(weights, returned.reshape(capacity, piece)).astype(jnp.bfloat16)

    pieces = combined.reshape(tp_size, rows_here // tp_size, piece)
    arrived = exchange(pieces, "tp")
    arrived = arrived.reshape(tp_size // PARTS, PARTS, rows_here // tp_size, piece)
    arrived = sum(arrived[i].astype(jnp.float32) for i in range(tp_size // PARTS))
    skip = PARTS * piece - width
    parts = [arrived[i] for i in range(PARTS)]
    parts[-1] = parts[-1][:, skip:]
    return jnp.concatenate(parts, 1).astype(jnp.bfloat16)


def solution(mesh):
    in_specs = (
        P(("ep", "dp"), None),
        P(("ep", "dp"), None),
        P(("ep", "dp"), None),
        P("ep", None, "tp"),
        P("ep", None, "tp"),
        P("ep", "tp", None),
    )
    out_specs = P(("ep", "dp", "tp"), None)
    return jax.shard_map(
        per_device, mesh=mesh, in_specs=in_specs, out_specs=out_specs, check_vma=False
    )
```

```python
import jax
import jax.numpy as jnp
from jax import lax
from jax.experimental import pallas as pl
from jax.experimental.pallas import tpu as pltpu
from jax.sharding import PartitionSpec as P

TOP = 8
EXPERTS = 32
MOST = 8
LANES = 128
PARTS = 3
BACK = 4
BLOCK = 5 * LANES


def shift(array, step):
    size = lax.axis_size("tp")
    pairs = [
        (core * size + i, core * size + (i + sign * step) % size)
        for core, sign in ((0, 1), (1, -1))
        for i in range(size)
    ]
    return lax.ppermute(array, ("dp", "tp"), pairs)


def swap(array):
    return lax.ppermute(array, "dp", [(0, 1), (1, 0)])


def exchange(array, axis):
    return lax.all_to_all(array, axis, split_axis=0, concat_axis=0, tiled=True)


def hop_two(array):
    size = lax.axis_size("tp")
    return lax.ppermute(
        array, "tp", [(i, (i + (2 if i % 2 else size - 2)) % size) for i in range(size)]
    )


def piece_width(width):
    tiles = -(-width // LANES)
    return -(-tiles // PARTS) * LANES


def piece_start(index, width):
    piece = piece_width(width)
    return jnp.minimum(lax.rem(index, PARTS) * piece, width - piece)


def cut_gate_up(start_ref, gate_ref, up_ref, out_ref, sem):
    piece, units = out_ref.shape[0], gate_ref.shape[2]
    rows = pl.ds(pl.multiple_of(start_ref[0], LANES), piece)
    copies = [
        pltpu.make_async_copy(
            ref.at[0, rows, :], out_ref.at[:, pl.ds(i * units, units)], sem.at[i]
        )
        for i, ref in enumerate((gate_ref, up_ref))
    ]
    for copy in copies:
        copy.start()
    for copy in copies:
        copy.wait()


def cut_down(start_ref, down_ref, out_ref, sem):
    columns = pl.ds(pl.multiple_of(start_ref[0], LANES), out_ref.shape[1])
    copy = pltpu.make_async_copy(down_ref.at[0, :, columns], out_ref, sem.at[0])
    copy.start()
    copy.wait()


def cut(kernel, start, arrays, shape):
    size = shape[0] * shape[1]
    return pl.pallas_call(
        kernel,
        out_shape=jax.ShapeDtypeStruct(shape, jnp.bfloat16),
        in_specs=[pl.BlockSpec(memory_space=pltpu.SMEM)]
        + [pl.BlockSpec(memory_space=pl.ANY)] * len(arrays),
        out_specs=pl.BlockSpec(memory_space=pltpu.VMEM),
        scratch_shapes=[pltpu.SemaphoreType.DMA((2,))],
        cost_estimate=pl.CostEstimate(
            flops=500 * size, bytes_accessed=4 * size, transcendentals=0
        ),
    )(start.reshape(1), *arrays)


def gate_up_piece(gate_weight, up_weight, index):
    width, units = gate_weight.shape[1:]
    shape = (piece_width(width), 2 * units)
    return cut(cut_gate_up, piece_start(index, width), (gate_weight, up_weight), shape)


def down_piece(down_weight, index, half=None):
    units, width = down_weight.shape[1:]
    size = width // BACK
    start = lax.rem(index, BACK) * size
    if half is not None:
        size //= 2
        start = start + half * size
    return cut(cut_down, start, (down_weight,), (units, size))


def dispatch_kernel(start_ref, ids_ref, tokens_ref, rows_ref, ids, held, chosen, sem):
    capacity, count = chosen.shape
    width = tokens_ref.shape[1]
    piece = piece_width(width)
    block = rows_ref.shape[1]
    step = pl.program_id(0)

    @pl.when(step == 0)
    def _():
        ids_copy = pltpu.make_async_copy(ids_ref, ids, sem.at[1])
        ids_copy.start()
        start = pl.multiple_of(start_ref[0], LANES)
        copy = pltpu.make_async_copy(
            tokens_ref.at[:, pl.ds(start, piece)], held.at[:, pl.ds(0, piece)], sem.at[0]
        )
        copy.start()
        line = lax.broadcasted_iota(jnp.int32, (capacity, count), 0)
        expert, slot = line // MOST, line % MOST
        member = jnp.zeros((capacity, count), jnp.float32)
        ids_copy.wait()
        for k in range(TOP):
            member = jnp.where(ids[k : k + 1, :] == expert, 1.0, member)
        row = lax.broadcasted_iota(jnp.int32, (count, count), 0)
        column = lax.broadcasted_iota(jnp.int32, (count, count), 1)
        before = jnp.where(row < column, 1.0, 0.0).astype(jnp.bfloat16)
        earlier = jnp.dot(member.astype(jnp.bfloat16), before, preferred_element_type=jnp.float32)
        here = earlier == slot.astype(jnp.float32)
        chosen[...] = jnp.where(here, member, 0.0).astype(jnp.bfloat16)
        copy.wait()

    first = jnp.where(start_ref[0] == width - piece, PARTS * piece - width, 0)
    source = held[:, pl.ds(pl.multiple_of(step * block, LANES), block)]
    wide = lax.broadcasted_iota(jnp.int32, source.shape, 1) + step * block
    source = jnp.where(wide >= first, source.astype(jnp.float32), 0.0).astype(jnp.bfloat16)
    rows_ref[...] = jnp.dot(chosen[...], source, preferred_element_type=jnp.float32).astype(
        jnp.bfloat16
    )


def dispatch(tokens, expert_ids, index):
    count, width = tokens.shape
    piece, capacity = piece_width(width), EXPERTS * MOST
    steps = -(-piece // BLOCK)
    return pl.pallas_call(
        dispatch_kernel,
        grid=(steps,),
        out_shape=jax.ShapeDtypeStruct((capacity, piece), jnp.bfloat16),
        in_specs=[
            pl.BlockSpec(memory_space=pltpu.SMEM),
            pl.BlockSpec(memory_space=pl.ANY),
            pl.BlockSpec(memory_space=pl.ANY),
        ],
        out_specs=pl.BlockSpec((capacity, BLOCK), lambda i: (0, i)),
        scratch_shapes=[
            pltpu.VMEM((TOP, count), jnp.int32),
            pltpu.VMEM((count, steps * BLOCK), jnp.bfloat16),
            pltpu.VMEM((capacity, count), jnp.bfloat16),
            pltpu.SemaphoreType.DMA((2,)),
        ],
        cost_estimate=pl.CostEstimate(
            flops=2 * count * piece * capacity, bytes_accessed=2**21, transcendentals=0
        ),
        name="dispatch",
    )(piece_start(index, width).reshape(1), expert_ids.T, tokens)


def weigh_kernel(ids_ref, route_ref, weights_ref):
    count, capacity = weights_ref.shape[1:]
    lane = lax.broadcasted_iota(jnp.int32, (count, capacity), 1)
    expert, slot = lane // MOST, lane % MOST
    member = jnp.zeros((count, capacity), jnp.float32)
    weight = jnp.zeros((count, capacity), jnp.float32)
    for k in range(TOP):
        same = ids_ref[:, k : k + 1] == expert
        member = jnp.where(same, 1.0, member)
        weight = jnp.where(same, route_ref[:, k : k + 1], weight)
    row = lax.broadcasted_iota(jnp.int32, (count, count), 0)
    column = lax.broadcasted_iota(jnp.int32, (count, count), 1)
    above = jnp.where(column < row, 1.0, 0.0).astype(jnp.bfloat16)
    earlier = jnp.dot(above, member.astype(jnp.bfloat16), preferred_element_type=jnp.float32)
    weight = jnp.where(earlier == slot.astype(jnp.float32), weight, 0.0)
    high = weight.astype(jnp.bfloat16)
    weights_ref[0] = high
    weights_ref[1] = (weight - high.astype(jnp.float32)).astype(jnp.bfloat16)


def weigh(expert_ids, route_weight):
    shape = (2, expert_ids.shape[0], EXPERTS * MOST)
    return pl.pallas_call(
        weigh_kernel,
        out_shape=jax.ShapeDtypeStruct(shape, jnp.bfloat16),
        cost_estimate=pl.CostEstimate(
            flops=2**26, bytes_accessed=2**15, transcendentals=0
        ),
        name="weigh",
    )(expert_ids, route_weight)


def combine(weights, returned):
    parts, rows, capacity = weights.shape
    both = weights.reshape(parts * rows, capacity)
    sums = jnp.dot(both, returned, preferred_element_type=jnp.float32)
    return sums[:rows] + sums[rows:]


def per_device(tokens, expert_ids, route_weight, gate_weight, up_weight, down_weight):
    rows_here, width = tokens.shape
    piece = piece_width(width)
    units = gate_weight.shape[2]
    capacity = EXPERTS * MOST
    tp_size = lax.axis_size("tp")
    here = lax.axis_index("tp")
    core = lax.axis_index("dp")
    target = lax.rem(here + jnp.where(core == 0, 1, tp_size - 1), tp_size)
    target_two = lax.rem(here + jnp.where(lax.rem(here, 2) == 0, tp_size - 2, 2), tp_size)

    outgoing = dispatch(tokens, expert_ids, here)
    outgoing, gate_weight, up_weight, down_weight, expert_ids, route_weight = (
        lax.optimization_barrier(
            (outgoing, gate_weight, up_weight, down_weight, expert_ids, route_weight)
        )
    )
    received = exchange(outgoing.reshape(EXPERTS, MOST, piece), "ep")
    received = received.reshape(capacity, piece)

    gate_up_near = shift(gate_up_piece(gate_weight, up_weight, target), 1)
    gate_up_far = swap(gate_up_near)
    down_near = shift(down_piece(down_weight, target), 1)
    down_far = swap(down_near)
    mine = hop_two(down_piece(down_weight, target_two, core))
    other = swap(mine)
    down_two = jnp.concatenate(
        [jnp.where(core == 0, mine, other), jnp.where(core == 0, other, mine)], 1
    )
    gate_up_here = gate_up_piece(gate_weight, up_weight, here)
    down_here = down_piece(down_weight, here)
    weights = weigh(expert_ids, route_weight)

    def product(weights):
        return jnp.dot(received, weights, preferred_element_type=jnp.float32)

    from_far = shift(product(gate_up_near).astype(jnp.bfloat16), -1)
    from_near = shift(product(gate_up_far).astype(jnp.bfloat16), 1)
    gate_up = product(gate_up_here)
    gate_up = gate_up + from_far.astype(jnp.float32) + from_near.astype(jnp.float32)
    hidden = (jax.nn.silu(gate_up[:, :units]) * gate_up[:, units:]).astype(jnp.bfloat16)
    hidden_near, hidden_far, hidden_two = shift(hidden, 1), shift(hidden, -1), hop_two(hidden)
    partial_rows = jnp.dot(
        jnp.concatenate([hidden_near, hidden, hidden_far, hidden_two], 1),
        jnp.concatenate([down_near, down_here, down_far, down_two], 0),
        preferred_element_type=jnp.float32,
    ).astype(jnp.bfloat16)
    size = width // BACK
    returned = exchange(partial_rows.reshape(EXPERTS, MOST, size), "ep")
    combined = combine(weights, returned.reshape(capacity, size)).astype(jnp.bfloat16)

    arrived = exchange(combined.reshape(tp_size, rows_here // tp_size, size), "tp")
    arrived = arrived.reshape(tp_size // BACK, BACK, rows_here // tp_size, size)
    arrived = sum(arrived[i].astype(jnp.float32) for i in range(tp_size // BACK))
    return jnp.concatenate([arrived[i] for i in range(BACK)], 1).astype(jnp.bfloat16)


def solution(mesh):
    in_specs = (
        P(("ep", "dp"), None),
        P(("ep", "dp"), None),
        P(("ep", "dp"), None),
        P("ep", None, "tp"),
        P("ep", None, "tp"),
        P("ep", "tp", None),
    )
    out_specs = P(("ep", "dp", "tp"), None)
    return jax.shard_map(
        per_device, mesh=mesh, in_specs=in_specs, out_specs=out_specs, check_vma=False
    )
```

```python
import jax
import jax.numpy as jnp
from jax import lax
from jax.experimental import pallas as pl
from jax.experimental.pallas import tpu as pltpu
from jax.sharding import PartitionSpec as P

TOP = 8
EXPERTS = 32
MOST = 8
LANES = 128
PARTS = 3
BACK = 4
STRIPS = 4
BLOCK = 5 * LANES


def shift(array, step):
    size = lax.axis_size("tp")
    pairs = [
        (core * size + i, core * size + (i + sign * step) % size)
        for core, sign in ((0, 1), (1, -1))
        for i in range(size)
    ]
    return lax.ppermute(array, ("dp", "tp"), pairs)


def swap(array):
    return lax.ppermute(array, "dp", [(0, 1), (1, 0)])


def exchange(array, axis):
    return lax.all_to_all(array, axis, split_axis=0, concat_axis=0, tiled=True)


def hop_two(array):
    size = lax.axis_size("tp")
    return lax.ppermute(
        array, "tp", [(i, (i + (2 if i % 2 else size - 2)) % size) for i in range(size)]
    )


def piece_width(width):
    tiles = -(-width // LANES)
    return -(-tiles // PARTS) * LANES


def piece_start(index, width):
    piece = piece_width(width)
    return jnp.minimum(lax.rem(index, PARTS) * piece, width - piece)


def cut_gate_up(start_ref, gate_ref, up_ref, out_ref, held, in_sem, out_sem):
    piece, units = out_ref.shape[0], gate_ref.shape[2]
    rows = piece // STRIPS
    arriving, leaving = [], []
    for strip in range(STRIPS):
        source = pl.ds(pl.multiple_of(start_ref[0] + strip * rows, 16), rows)
        target = pl.ds(strip * rows, rows)
        arriving.append(
            [
                pltpu.make_async_copy(
                    ref.at[0, source, :],
                    held.at[target, pl.ds(i * units, units)],
                    in_sem.at[strip, i],
                )
                for i, ref in enumerate((gate_ref, up_ref))
            ]
        )
        leaving.append(
            pltpu.make_async_copy(held.at[target, :], out_ref.at[target, :], out_sem.at[strip])
        )
    for pair in arriving:
        for copy in pair:
            copy.start()
    for pair, out in zip(arriving, leaving):
        for copy in pair:
            copy.wait()
        out.start()
    for out in leaving:
        out.wait()


def cut_down(start_ref, down_ref, out_ref, sem):
    columns = pl.ds(pl.multiple_of(start_ref[0], LANES), out_ref.shape[1])
    copy = pltpu.make_async_copy(down_ref.at[0, :, columns], out_ref, sem.at[0])
    copy.start()
    copy.wait()


def cut(kernel, start, arrays, shape, out_space, scratch):
    size = shape[0] * shape[1]
    return pl.pallas_call(
        kernel,
        out_shape=jax.ShapeDtypeStruct(shape, jnp.bfloat16),
        in_specs=[pl.BlockSpec(memory_space=pltpu.SMEM)]
        + [pl.BlockSpec(memory_space=pl.ANY)] * len(arrays),
        out_specs=pl.BlockSpec(memory_space=out_space),
        scratch_shapes=scratch,
        cost_estimate=pl.CostEstimate(
            flops=500 * size, bytes_accessed=4 * size, transcendentals=0
        ),
    )(start.reshape(1), *arrays)


def gate_up_piece(gate_weight, up_weight, index):
    width, units = gate_weight.shape[1:]
    shape = (piece_width(width), 2 * units)
    scratch = [
        pltpu.VMEM(shape, jnp.bfloat16),
        pltpu.SemaphoreType.DMA((STRIPS, 2)),
        pltpu.SemaphoreType.DMA((STRIPS,)),
    ]
    arrays = (gate_weight, up_weight)
    return cut(cut_gate_up, piece_start(index, width), arrays, shape, pl.ANY, scratch)


def down_piece(down_weight, index, half=None):
    units, width = down_weight.shape[1:]
    size = width // BACK
    start = lax.rem(index, BACK) * size
    if half is not None:
        size //= 2
        start = start + half * size
    scratch = [pltpu.SemaphoreType.DMA((1,))]
    return cut(cut_down, start, (down_weight,), (units, size), pltpu.VMEM, scratch)


def dispatch_kernel(start_ref, ids_ref, tokens_ref, rows_ref, ids, held, chosen, sem):
    capacity, count = chosen.shape
    width = tokens_ref.shape[1]
    piece = piece_width(width)
    block = rows_ref.shape[1]
    step = pl.program_id(0)

    @pl.when(step == 0)
    def _():
        ids_copy = pltpu.make_async_copy(ids_ref, ids, sem.at[1])
        ids_copy.start()
        start = pl.multiple_of(start_ref[0], LANES)
        copy = pltpu.make_async_copy(
            tokens_ref.at[:, pl.ds(start, piece)], held.at[:, pl.ds(0, piece)], sem.at[0]
        )
        copy.start()
        line = lax.broadcasted_iota(jnp.int32, (capacity, count), 0)
        expert, slot = line // MOST, line % MOST
        member = jnp.zeros((capacity, count), jnp.float32)
        ids_copy.wait()
        for k in range(TOP):
            member = jnp.where(ids[k : k + 1, :] == expert, 1.0, member)
        row = lax.broadcasted_iota(jnp.int32, (count, count), 0)
        column = lax.broadcasted_iota(jnp.int32, (count, count), 1)
        before = jnp.where(row < column, 1.0, 0.0).astype(jnp.bfloat16)
        earlier = jnp.dot(member.astype(jnp.bfloat16), before, preferred_element_type=jnp.float32)
        here = earlier == slot.astype(jnp.float32)
        chosen[...] = jnp.where(here, member, 0.0).astype(jnp.bfloat16)
        copy.wait()

    first = jnp.where(start_ref[0] == width - piece, PARTS * piece - width, 0)
    source = held[:, pl.ds(pl.multiple_of(step * block, LANES), block)]
    wide = lax.broadcasted_iota(jnp.int32, source.shape, 1) + step * block
    source = jnp.where(wide >= first, source.astype(jnp.float32), 0.0).astype(jnp.bfloat16)
    rows_ref[...] = jnp.dot(chosen[...], source, preferred_element_type=jnp.float32).astype(
        jnp.bfloat16
    )


def dispatch(tokens, expert_ids, index):
    count, width = tokens.shape
    piece, capacity = piece_width(width), EXPERTS * MOST
    steps = -(-piece // BLOCK)
    return pl.pallas_call(
        dispatch_kernel,
        grid=(steps,),
        out_shape=jax.ShapeDtypeStruct((capacity, piece), jnp.bfloat16),
        in_specs=[
            pl.BlockSpec(memory_space=pltpu.SMEM),
            pl.BlockSpec(memory_space=pl.ANY),
            pl.BlockSpec(memory_space=pl.ANY),
        ],
        out_specs=pl.BlockSpec((capacity, BLOCK), lambda i: (0, i)),
        scratch_shapes=[
            pltpu.VMEM((TOP, count), jnp.int32),
            pltpu.VMEM((count, steps * BLOCK), jnp.bfloat16),
            pltpu.VMEM((capacity, count), jnp.bfloat16),
            pltpu.SemaphoreType.DMA((2,)),
        ],
        cost_estimate=pl.CostEstimate(
            flops=2 * count * piece * capacity, bytes_accessed=2**21, transcendentals=0
        ),
        name="dispatch",
    )(piece_start(index, width).reshape(1), expert_ids.T, tokens)


def weigh_kernel(ids_ref, route_ref, weights_ref):
    count, capacity = weights_ref.shape[1:]
    lane = lax.broadcasted_iota(jnp.int32, (count, capacity), 1)
    expert, slot = lane // MOST, lane % MOST
    member = jnp.zeros((count, capacity), jnp.float32)
    weight = jnp.zeros((count, capacity), jnp.float32)
    for k in range(TOP):
        same = ids_ref[:, k : k + 1] == expert
        member = jnp.where(same, 1.0, member)
        weight = jnp.where(same, route_ref[:, k : k + 1], weight)
    row = lax.broadcasted_iota(jnp.int32, (count, count), 0)
    column = lax.broadcasted_iota(jnp.int32, (count, count), 1)
    above = jnp.where(column < row, 1.0, 0.0).astype(jnp.bfloat16)
    earlier = jnp.dot(above, member.astype(jnp.bfloat16), preferred_element_type=jnp.float32)
    weight = jnp.where(earlier == slot.astype(jnp.float32), weight, 0.0)
    high = weight.astype(jnp.bfloat16)
    weights_ref[0] = high
    weights_ref[1] = (weight - high.astype(jnp.float32)).astype(jnp.bfloat16)


def weigh(expert_ids, route_weight):
    shape = (2, expert_ids.shape[0], EXPERTS * MOST)
    return pl.pallas_call(
        weigh_kernel,
        out_shape=jax.ShapeDtypeStruct(shape, jnp.bfloat16),
        cost_estimate=pl.CostEstimate(
            flops=2**26, bytes_accessed=2**15, transcendentals=0
        ),
        name="weigh",
    )(expert_ids, route_weight)


def combine(weights, returned):
    parts, rows, capacity = weights.shape
    both = weights.reshape(parts * rows, capacity)
    sums = jnp.dot(both, returned, preferred_element_type=jnp.float32)
    return sums[:rows] + sums[rows:]


def per_device(tokens, expert_ids, route_weight, gate_weight, up_weight, down_weight):
    rows_here, width = tokens.shape
    piece = piece_width(width)
    units = gate_weight.shape[2]
    capacity = EXPERTS * MOST
    tp_size = lax.axis_size("tp")
    here = lax.axis_index("tp")
    core = lax.axis_index("dp")
    target = lax.rem(here + jnp.where(core == 0, 1, tp_size - 1), tp_size)
    target_two = lax.rem(here + jnp.where(lax.rem(here, 2) == 0, tp_size - 2, 2), tp_size)

    outgoing = dispatch(tokens, expert_ids, here)
    outgoing, gate_weight, up_weight, down_weight, expert_ids, route_weight = (
        lax.optimization_barrier(
            (outgoing, gate_weight, up_weight, down_weight, expert_ids, route_weight)
        )
    )
    received = exchange(outgoing.reshape(EXPERTS, MOST, piece), "ep")
    received = received.reshape(capacity, piece)

    gate_up_near = shift(gate_up_piece(gate_weight, up_weight, target), 1)
    gate_up_far = swap(gate_up_near)
    down_near = shift(down_piece(down_weight, target), 1)
    down_far = swap(down_near)
    mine = hop_two(down_piece(down_weight, target_two, core))
    other = swap(mine)
    down_two = jnp.concatenate(
        [jnp.where(core == 0, mine, other), jnp.where(core == 0, other, mine)], 1
    )
    gate_up_here = gate_up_piece(gate_weight, up_weight, here)
    down_here = down_piece(down_weight, here)
    weights = weigh(expert_ids, route_weight)

    def product(weights):
        return jnp.dot(received, weights, preferred_element_type=jnp.float32)

    from_far = shift(product(gate_up_near).astype(jnp.bfloat16), -1)
    from_near = shift(product(gate_up_far).astype(jnp.bfloat16), 1)
    gate_up = product(gate_up_here)
    gate_up = gate_up + from_far.astype(jnp.float32) + from_near.astype(jnp.float32)
    hidden = (jax.nn.silu(gate_up[:, :units]) * gate_up[:, units:]).astype(jnp.bfloat16)
    hidden_two = hop_two(hidden)
    hidden_near = shift(hidden, 1)
    hidden_far = shift(hidden, -1)
    partial_rows = jnp.dot(
        jnp.concatenate([hidden_near, hidden, hidden_far, hidden_two], 1),
        jnp.concatenate([down_near, down_here, down_far, down_two], 0),
        preferred_element_type=jnp.float32,
    ).astype(jnp.bfloat16)
    size = width // BACK
    returned = exchange(partial_rows.reshape(EXPERTS, MOST, size), "ep")
    combined = combine(weights, returned.reshape(capacity, size)).astype(jnp.bfloat16)

    arrived = exchange(combined.reshape(tp_size, rows_here // tp_size, size), "tp")
    arrived = arrived.reshape(tp_size // BACK, BACK, rows_here // tp_size, size)
    arrived = sum(arrived[i].astype(jnp.float32) for i in range(tp_size // BACK))
    return jnp.concatenate([arrived[i] for i in range(BACK)], 1).astype(jnp.bfloat16)


def solution(mesh):
    in_specs = (
        P(("ep", "dp"), None),
        P(("ep", "dp"), None),
        P(("ep", "dp"), None),
        P("ep", None, "tp"),
        P("ep", None, "tp"),
        P("ep", "tp", None),
    )
    out_specs = P(("ep", "dp", "tp"), None)
    return jax.shard_map(
        per_device, mesh=mesh, in_specs=in_specs, out_specs=out_specs, check_vma=False
    )
```

```python
import jax
import jax.numpy as jnp
from jax import lax
from jax.experimental import pallas as pl
from jax.experimental.pallas import tpu as pltpu
from jax.sharding import PartitionSpec as P

TOP = 8
EXPERTS = 32
MOST = 8
LANES = 128
PARTS = 3
BACK = 4
STRIPS = 4
BLOCK = 5 * LANES


def shift(array, step):
    size = lax.axis_size("tp")
    pairs = [
        (core * size + i, core * size + (i + sign * step) % size)
        for core, sign in ((0, 1), (1, -1))
        for i in range(size)
    ]
    return lax.ppermute(array, ("dp", "tp"), pairs)


def swap(array):
    return lax.ppermute(array, "dp", [(0, 1), (1, 0)])


def exchange(array, axis):
    return lax.all_to_all(array, axis, split_axis=0, concat_axis=0, tiled=True)


def piece_width(width):
    tiles = -(-width // LANES)
    return -(-tiles // PARTS) * LANES


def piece_start(index, width):
    piece = piece_width(width)
    return jnp.minimum(lax.rem(index, PARTS) * piece, width - piece)


def cut_gate_up(start_ref, gate_ref, up_ref, out_ref, held, in_sem, out_sem):
    piece, units = out_ref.shape[0], gate_ref.shape[2]
    rows = piece // STRIPS
    arriving, leaving = [], []
    for strip in range(STRIPS):
        source = pl.ds(pl.multiple_of(start_ref[0] + strip * rows, 16), rows)
        target = pl.ds(strip * rows, rows)
        arriving.append(
            [
                pltpu.make_async_copy(
                    ref.at[0, source, :],
                    held.at[target, pl.ds(i * units, units)],
                    in_sem.at[strip, i],
                )
                for i, ref in enumerate((gate_ref, up_ref))
            ]
        )
        leaving.append(
            pltpu.make_async_copy(held.at[target, :], out_ref.at[target, :], out_sem.at[strip])
        )
    for pair in arriving:
        for copy in pair:
            copy.start()
    for pair, out in zip(arriving, leaving):
        for copy in pair:
            copy.wait()
        out.start()
    for out in leaving:
        out.wait()


def cut_down(start_ref, down_ref, out_ref, sem):
    columns = pl.ds(pl.multiple_of(start_ref[0], LANES), out_ref.shape[1])
    copy = pltpu.make_async_copy(down_ref.at[0, :, columns], out_ref, sem.at[0])
    copy.start()
    copy.wait()


def cut(kernel, start, arrays, shape, out_space, scratch):
    size = shape[0] * shape[1]
    return pl.pallas_call(
        kernel,
        out_shape=jax.ShapeDtypeStruct(shape, jnp.bfloat16),
        in_specs=[pl.BlockSpec(memory_space=pltpu.SMEM)]
        + [pl.BlockSpec(memory_space=pl.ANY)] * len(arrays),
        out_specs=pl.BlockSpec(memory_space=out_space),
        scratch_shapes=scratch,
        cost_estimate=pl.CostEstimate(
            flops=500 * size, bytes_accessed=4 * size, transcendentals=0
        ),
    )(start.reshape(1), *arrays)


def gate_up_piece(gate_weight, up_weight, index):
    width, units = gate_weight.shape[1:]
    shape = (piece_width(width), 2 * units)
    scratch = [
        pltpu.VMEM(shape, jnp.bfloat16),
        pltpu.SemaphoreType.DMA((STRIPS, 2)),
        pltpu.SemaphoreType.DMA((STRIPS,)),
    ]
    arrays = (gate_weight, up_weight)
    return cut(cut_gate_up, piece_start(index, width), arrays, shape, pl.ANY, scratch)


def down_piece(down_weight, index):
    units, width = down_weight.shape[1:]
    size = width // BACK
    start = lax.rem(index, BACK) * size
    scratch = [pltpu.SemaphoreType.DMA((1,))]
    return cut(cut_down, start, (down_weight,), (units, size), pltpu.VMEM, scratch)


def dispatch_kernel(start_ref, ids_ref, tokens_ref, rows_ref, ids, held, chosen, sem):
    capacity, count = chosen.shape
    width = tokens_ref.shape[1]
    piece = piece_width(width)
    block = rows_ref.shape[1]
    step = pl.program_id(0)

    @pl.when(step == 0)
    def _():
        ids_copy = pltpu.make_async_copy(ids_ref, ids, sem.at[1])
        ids_copy.start()
        start = pl.multiple_of(start_ref[0], LANES)
        copy = pltpu.make_async_copy(
            tokens_ref.at[:, pl.ds(start, piece)], held.at[:, pl.ds(0, piece)], sem.at[0]
        )
        copy.start()
        line = lax.broadcasted_iota(jnp.int32, (capacity, count), 0)
        expert, slot = line // MOST, line % MOST
        member = jnp.zeros((capacity, count), jnp.float32)
        ids_copy.wait()
        for k in range(TOP):
            member = jnp.where(ids[k : k + 1, :] == expert, 1.0, member)
        row = lax.broadcasted_iota(jnp.int32, (count, count), 0)
        column = lax.broadcasted_iota(jnp.int32, (count, count), 1)
        before = jnp.where(row < column, 1.0, 0.0).astype(jnp.bfloat16)
        earlier = jnp.dot(member.astype(jnp.bfloat16), before, preferred_element_type=jnp.float32)
        here = earlier == slot.astype(jnp.float32)
        chosen[...] = jnp.where(here, member, 0.0).astype(jnp.bfloat16)
        copy.wait()

    first = jnp.where(start_ref[0] == width - piece, PARTS * piece - width, 0)
    source = held[:, pl.ds(pl.multiple_of(step * block, LANES), block)]
    wide = lax.broadcasted_iota(jnp.int32, source.shape, 1) + step * block
    source = jnp.where(wide >= first, source.astype(jnp.float32), 0.0).astype(jnp.bfloat16)
    rows_ref[...] = jnp.dot(chosen[...], source, preferred_element_type=jnp.float32).astype(
        jnp.bfloat16
    )


def dispatch(tokens, expert_ids, index):
    count, width = tokens.shape
    piece, capacity = piece_width(width), EXPERTS * MOST
    steps = -(-piece // BLOCK)
    return pl.pallas_call(
        dispatch_kernel,
        grid=(steps,),
        out_shape=jax.ShapeDtypeStruct((capacity, piece), jnp.bfloat16),
        in_specs=[
            pl.BlockSpec(memory_space=pltpu.SMEM),
            pl.BlockSpec(memory_space=pl.ANY),
            pl.BlockSpec(memory_space=pl.ANY),
        ],
        out_specs=pl.BlockSpec((capacity, BLOCK), lambda i: (0, i)),
        scratch_shapes=[
            pltpu.VMEM((TOP, count), jnp.int32),
            pltpu.VMEM((count, steps * BLOCK), jnp.bfloat16),
            pltpu.VMEM((capacity, count), jnp.bfloat16),
            pltpu.SemaphoreType.DMA((2,)),
        ],
        cost_estimate=pl.CostEstimate(
            flops=2 * count * piece * capacity, bytes_accessed=2**21, transcendentals=0
        ),
        name="dispatch",
    )(piece_start(index, width).reshape(1), expert_ids.T, tokens)


def weigh_kernel(ids_ref, route_ref, weights_ref):
    count, capacity = weights_ref.shape[1:]
    lane = lax.broadcasted_iota(jnp.int32, (count, capacity), 1)
    expert, slot = lane // MOST, lane % MOST
    member = jnp.zeros((count, capacity), jnp.float32)
    weight = jnp.zeros((count, capacity), jnp.float32)
    for k in range(TOP):
        same = ids_ref[:, k : k + 1] == expert
        member = jnp.where(same, 1.0, member)
        weight = jnp.where(same, route_ref[:, k : k + 1], weight)
    row = lax.broadcasted_iota(jnp.int32, (count, count), 0)
    column = lax.broadcasted_iota(jnp.int32, (count, count), 1)
    above = jnp.where(column < row, 1.0, 0.0).astype(jnp.bfloat16)
    earlier = jnp.dot(above, member.astype(jnp.bfloat16), preferred_element_type=jnp.float32)
    weight = jnp.where(earlier == slot.astype(jnp.float32), weight, 0.0)
    high = weight.astype(jnp.bfloat16)
    weights_ref[0] = high
    weights_ref[1] = (weight - high.astype(jnp.float32)).astype(jnp.bfloat16)


def weigh(expert_ids, route_weight):
    shape = (2, expert_ids.shape[0], EXPERTS * MOST)
    return pl.pallas_call(
        weigh_kernel,
        out_shape=jax.ShapeDtypeStruct(shape, jnp.bfloat16),
        cost_estimate=pl.CostEstimate(
            flops=2**26, bytes_accessed=2**15, transcendentals=0
        ),
        name="weigh",
    )(expert_ids, route_weight)


def combine(weights, returned):
    parts, rows, capacity = weights.shape
    both = weights.reshape(parts * rows, capacity)
    sums = jnp.dot(both, returned, preferred_element_type=jnp.float32)
    return sums[:rows] + sums[rows:]


def per_device(tokens, expert_ids, route_weight, gate_weight, up_weight, down_weight):
    rows_here, width = tokens.shape
    piece = piece_width(width)
    units = gate_weight.shape[2]
    capacity = EXPERTS * MOST
    tp_size = lax.axis_size("tp")
    here = lax.axis_index("tp")
    core = lax.axis_index("dp")
    target = lax.rem(here + jnp.where(core == 0, 1, tp_size - 1), tp_size)
    target_two = lax.rem(here + jnp.where(core == 0, tp_size - 2, 2), tp_size)

    outgoing = dispatch(tokens, expert_ids, here)
    outgoing, gate_weight, up_weight, down_weight, expert_ids, route_weight = (
        lax.optimization_barrier(
            (outgoing, gate_weight, up_weight, down_weight, expert_ids, route_weight)
        )
    )
    received = exchange(outgoing.reshape(EXPERTS, MOST, piece), "ep")
    received = received.reshape(capacity, piece)

    gate_up_near = shift(gate_up_piece(gate_weight, up_weight, target), 1)
    gate_up_far = swap(gate_up_near)
    down_near = shift(down_piece(down_weight, target), 1)
    down_far = swap(down_near)
    down_two = shift(down_piece(down_weight, target_two), -2)
    gate_up_here = gate_up_piece(gate_weight, up_weight, here)
    down_here = down_piece(down_weight, here)
    weights = weigh(expert_ids, route_weight)

    def product(weights):
        return jnp.dot(received, weights, preferred_element_type=jnp.float32)

    from_far = shift(product(gate_up_near).astype(jnp.bfloat16), -1)
    from_near = shift(product(gate_up_far).astype(jnp.bfloat16), 1)
    gate_up = product(gate_up_here)
    gate_up = gate_up + from_far.astype(jnp.float32) + from_near.astype(jnp.float32)
    hidden = (jax.nn.silu(gate_up[:, :units]) * gate_up[:, units:]).astype(jnp.bfloat16)
    hidden_two = shift(hidden, -2)
    hidden_near = shift(hidden, 1)
    hidden_far = shift(hidden, -1)
    partial_rows = jnp.dot(
        jnp.concatenate([hidden_near, hidden, hidden_far, hidden_two], 1),
        jnp.concatenate([down_near, down_here, down_far, down_two], 0),
        preferred_element_type=jnp.float32,
    ).astype(jnp.bfloat16)
    size = width // BACK
    returned = exchange(partial_rows.reshape(EXPERTS, MOST, size), "ep")
    combined = combine(weights, returned.reshape(capacity, size)).astype(jnp.bfloat16)

    arrived = exchange(combined.reshape(tp_size, rows_here // tp_size, size), "tp")
    arrived = arrived.reshape(tp_size // BACK, BACK, rows_here // tp_size, size)
    arrived = sum(arrived[i].astype(jnp.float32) for i in range(tp_size // BACK))
    return jnp.concatenate([arrived[i] for i in range(BACK)], 1).astype(jnp.bfloat16)


def solution(mesh):
    in_specs = (
        P(("ep", "dp"), None),
        P(("ep", "dp"), None),
        P(("ep", "dp"), None),
        P("ep", None, "tp"),
        P("ep", None, "tp"),
        P("ep", "tp", None),
    )
    out_specs = P(("ep", "dp", "tp"), None)
    return jax.shard_map(
        per_device, mesh=mesh, in_specs=in_specs, out_specs=out_specs, check_vma=False
    )
```

```python
import jax
import jax.numpy as jnp
from jax import lax
from jax.experimental import pallas as pl
from jax.experimental.pallas import tpu as pltpu
from jax.sharding import PartitionSpec as P

TOP = 8
EXPERTS = 32
MOST = 8
LANES = 128
PARTS = 3
BACK = 4
STRIPS = 4
BLOCK = 5 * LANES


def shift(array, step):
    size = lax.axis_size("tp")
    pairs = [
        (core * size + i, core * size + (i + sign * step) % size)
        for core, sign in ((0, 1), (1, -1))
        for i in range(size)
    ]
    return lax.ppermute(array, ("dp", "tp"), pairs)


def swap(array):
    return lax.ppermute(array, "dp", [(0, 1), (1, 0)])


def exchange(array, axis):
    return lax.all_to_all(array, axis, split_axis=0, concat_axis=0, tiled=True)


def hop_two(array):
    size = lax.axis_size("tp")
    return lax.ppermute(
        array, "tp", [(i, (i + (2 if i % 2 else size - 2)) % size) for i in range(size)]
    )


def piece_width(width):
    tiles = -(-width // LANES)
    return -(-tiles // PARTS) * LANES


def piece_start(index, width):
    piece = piece_width(width)
    return jnp.minimum(lax.rem(index, PARTS) * piece, width - piece)


def cut_gate_up(start_ref, gate_ref, up_ref, out_ref, held, in_sem, out_sem):
    piece, units = out_ref.shape[0], gate_ref.shape[2]
    rows = piece // STRIPS
    arriving, leaving = [], []
    for strip in range(STRIPS):
        source = pl.ds(pl.multiple_of(start_ref[0] + strip * rows, 16), rows)
        target = pl.ds(strip * rows, rows)
        arriving.append(
            [
                pltpu.make_async_copy(
                    ref.at[0, source, :],
                    held.at[target, pl.ds(i * units, units)],
                    in_sem.at[strip, i],
                )
                for i, ref in enumerate((gate_ref, up_ref))
            ]
        )
        leaving.append(
            pltpu.make_async_copy(held.at[target, :], out_ref.at[target, :], out_sem.at[strip])
        )
    for pair in arriving:
        for copy in pair:
            copy.start()
    for pair, out in zip(arriving, leaving):
        for copy in pair:
            copy.wait()
        out.start()
    for out in leaving:
        out.wait()


def cut_down(start_ref, down_ref, out_ref, sem):
    columns = pl.ds(pl.multiple_of(start_ref[0], LANES), out_ref.shape[1])
    copy = pltpu.make_async_copy(down_ref.at[0, :, columns], out_ref, sem.at[0])
    copy.start()
    copy.wait()


def cut(kernel, start, arrays, shape, out_space, scratch):
    size = shape[0] * shape[1]
    return pl.pallas_call(
        kernel,
        out_shape=jax.ShapeDtypeStruct(shape, jnp.bfloat16),
        in_specs=[pl.BlockSpec(memory_space=pltpu.SMEM)]
        + [pl.BlockSpec(memory_space=pl.ANY)] * len(arrays),
        out_specs=pl.BlockSpec(memory_space=out_space),
        scratch_shapes=scratch,
        cost_estimate=pl.CostEstimate(
            flops=500 * size, bytes_accessed=4 * size, transcendentals=0
        ),
    )(start.reshape(1), *arrays)


def gate_up_piece(gate_weight, up_weight, index):
    width, units = gate_weight.shape[1:]
    shape = (piece_width(width), 2 * units)
    scratch = [
        pltpu.VMEM(shape, jnp.bfloat16),
        pltpu.SemaphoreType.DMA((STRIPS, 2)),
        pltpu.SemaphoreType.DMA((STRIPS,)),
    ]
    arrays = (gate_weight, up_weight)
    return cut(cut_gate_up, piece_start(index, width), arrays, shape, pl.ANY, scratch)


def down_piece(down_weight, index):
    units, width = down_weight.shape[1:]
    size = width // BACK
    scratch = [pltpu.SemaphoreType.DMA((1,))]
    start = lax.rem(index, BACK) * size
    return cut(cut_down, start, (down_weight,), (units, size), pltpu.VMEM, scratch)


def cut_own_kernel(
    gu_start, dn_start, two_start, gate_ref, up_ref, down_ref, gu_ref, dn_ref, two_ref,
    gu, dn, two, in_sem, out_sem, down_sem,
):
    piece, units = gu.shape[0], gate_ref.shape[2]
    rows = piece // STRIPS
    arriving, leaving = [], []
    for i, (start, held, out) in enumerate(((two_start, two, two_ref), (dn_start, dn, dn_ref))):
        columns = pl.ds(pl.multiple_of(start[0], LANES), held.shape[1])
        arriving.append(
            [pltpu.make_async_copy(down_ref.at[0, :, columns], held, down_sem.at[0, i])]
        )
        leaving.append(pltpu.make_async_copy(held, out, down_sem.at[1, i]))
    for strip in range(STRIPS):
        source = pl.ds(pl.multiple_of(gu_start[0] + strip * rows, 16), rows)
        target = pl.ds(strip * rows, rows)
        arriving.append(
            [
                pltpu.make_async_copy(
                    ref.at[0, source, :],
                    gu.at[target, pl.ds(i * units, units)],
                    in_sem.at[strip, i],
                )
                for i, ref in enumerate((gate_ref, up_ref))
            ]
        )
        leaving.append(
            pltpu.make_async_copy(gu.at[target, :], gu_ref.at[target, :], out_sem.at[strip])
        )
    for group in arriving:
        for copy in group:
            copy.start()
    for group, out in zip(arriving, leaving):
        for copy in group:
            copy.wait()
        out.start()
    for out in leaving:
        out.wait()


def cut_own(gate_weight, up_weight, down_weight, here, target_two, core):
    width, units = gate_weight.shape[1:]
    size = width // BACK
    shapes = ((piece_width(width), 2 * units), (units, size), (units, size // 2))
    starts = (
        piece_start(here, width),
        lax.rem(here, BACK) * size,
        lax.rem(target_two, BACK) * size + core * (size // 2),
    )
    total = sum(a * b for a, b in shapes)
    return pl.pallas_call(
        cut_own_kernel,
        out_shape=tuple(jax.ShapeDtypeStruct(shape, jnp.bfloat16) for shape in shapes),
        in_specs=[pl.BlockSpec(memory_space=pltpu.SMEM)] * 3
        + [pl.BlockSpec(memory_space=pl.ANY)] * 3,
        out_specs=(pl.BlockSpec(memory_space=pl.ANY),) * 3,
        scratch_shapes=[pltpu.VMEM(shape, jnp.bfloat16) for shape in shapes]
        + [
            pltpu.SemaphoreType.DMA((STRIPS, 2)),
            pltpu.SemaphoreType.DMA((STRIPS,)),
            pltpu.SemaphoreType.DMA((2, 2)),
        ],
        cost_estimate=pl.CostEstimate(
            flops=500 * total, bytes_accessed=4 * total, transcendentals=0
        ),
        name="cut_own",
    )(*(start.reshape(1) for start in starts), gate_weight, up_weight, down_weight)


def dispatch_kernel(start_ref, ids_ref, tokens_ref, rows_ref, ids, held, chosen, sem):
    capacity, count = chosen.shape
    width = tokens_ref.shape[1]
    piece = piece_width(width)
    block = rows_ref.shape[1]
    step = pl.program_id(0)

    @pl.when(step == 0)
    def _():
        ids_copy = pltpu.make_async_copy(ids_ref, ids, sem.at[1])
        ids_copy.start()
        start = pl.multiple_of(start_ref[0], LANES)
        copy = pltpu.make_async_copy(
            tokens_ref.at[:, pl.ds(start, piece)], held.at[:, pl.ds(0, piece)], sem.at[0]
        )
        copy.start()
        line = lax.broadcasted_iota(jnp.int32, (capacity, count), 0)
        expert, slot = line // MOST, line % MOST
        member = jnp.zeros((capacity, count), jnp.float32)
        ids_copy.wait()
        for k in range(TOP):
            member = jnp.where(ids[k : k + 1, :] == expert, 1.0, member)
        row = lax.broadcasted_iota(jnp.int32, (count, count), 0)
        column = lax.broadcasted_iota(jnp.int32, (count, count), 1)
        before = jnp.where(row < column, 1.0, 0.0).astype(jnp.bfloat16)
        earlier = jnp.dot(member.astype(jnp.bfloat16), before, preferred_element_type=jnp.float32)
        here = earlier == slot.astype(jnp.float32)
        chosen[...] = jnp.where(here, member, 0.0).astype(jnp.bfloat16)
        copy.wait()

    first = jnp.where(start_ref[0] == width - piece, PARTS * piece - width, 0)
    source = held[:, pl.ds(pl.multiple_of(step * block, LANES), block)]
    wide = lax.broadcasted_iota(jnp.int32, source.shape, 1) + step * block
    source = jnp.where(wide >= first, source.astype(jnp.float32), 0.0).astype(jnp.bfloat16)
    rows_ref[...] = jnp.dot(chosen[...], source, preferred_element_type=jnp.float32).astype(
        jnp.bfloat16
    )


def dispatch(tokens, expert_ids, index):
    count, width = tokens.shape
    piece, capacity = piece_width(width), EXPERTS * MOST
    steps = -(-piece // BLOCK)
    return pl.pallas_call(
        dispatch_kernel,
        grid=(steps,),
        out_shape=jax.ShapeDtypeStruct((capacity, piece), jnp.bfloat16),
        in_specs=[
            pl.BlockSpec(memory_space=pltpu.SMEM),
            pl.BlockSpec(memory_space=pl.ANY),
            pl.BlockSpec(memory_space=pl.ANY),
        ],
        out_specs=pl.BlockSpec((capacity, BLOCK), lambda i: (0, i)),
        scratch_shapes=[
            pltpu.VMEM((TOP, count), jnp.int32),
            pltpu.VMEM((count, steps * BLOCK), jnp.bfloat16),
            pltpu.VMEM((capacity, count), jnp.bfloat16),
            pltpu.SemaphoreType.DMA((2,)),
        ],
        cost_estimate=pl.CostEstimate(
            flops=2 * count * piece * capacity, bytes_accessed=2**21, transcendentals=0
        ),
        name="dispatch",
    )(piece_start(index, width).reshape(1), expert_ids.T, tokens)


def weigh_kernel(ids_ref, route_ref, weights_ref):
    capacity, count = weights_ref.shape[1:]
    line = lax.broadcasted_iota(jnp.int32, (capacity, count), 0)
    expert, slot = line // MOST, line % MOST
    member = jnp.zeros((capacity, count), jnp.float32)
    weight = jnp.zeros((capacity, count), jnp.float32)
    for k in range(TOP):
        same = ids_ref[k : k + 1, :] == expert
        member = jnp.where(same, 1.0, member)
        weight = jnp.where(same, route_ref[k : k + 1, :], weight)
    row = lax.broadcasted_iota(jnp.int32, (count, count), 0)
    column = lax.broadcasted_iota(jnp.int32, (count, count), 1)
    before = jnp.where(row < column, 1.0, 0.0).astype(jnp.bfloat16)
    earlier = jnp.dot(member.astype(jnp.bfloat16), before, preferred_element_type=jnp.float32)
    weight = jnp.where(earlier == slot.astype(jnp.float32), weight, 0.0)
    high = weight.astype(jnp.bfloat16)
    weights_ref[0] = high
    weights_ref[1] = (weight - high.astype(jnp.float32)).astype(jnp.bfloat16)


def weigh(expert_ids, route_weight):
    shape = (2, EXPERTS * MOST, expert_ids.shape[0])
    return pl.pallas_call(
        weigh_kernel,
        out_shape=jax.ShapeDtypeStruct(shape, jnp.bfloat16),
        cost_estimate=pl.CostEstimate(
            flops=2**26, bytes_accessed=2**15, transcendentals=0
        ),
        name="weigh",
    )(expert_ids.T, route_weight.T)


def combine(weights, returned):
    sums = jnp.einsum("ipt,pd->itd", weights, returned, preferred_element_type=jnp.float32)
    return sums[0] + sums[1]


def per_device(tokens, expert_ids, route_weight, gate_weight, up_weight, down_weight):
    rows_here, width = tokens.shape
    piece = piece_width(width)
    units = gate_weight.shape[2]
    capacity = EXPERTS * MOST
    tp_size = lax.axis_size("tp")
    here = lax.axis_index("tp")
    core = lax.axis_index("dp")
    target = lax.rem(here + jnp.where(core == 0, 1, tp_size - 1), tp_size)
    target_two = lax.rem(here + jnp.where(lax.rem(here, 2) == 0, tp_size - 2, 2), tp_size)

    outgoing = dispatch(tokens, expert_ids, here)
    outgoing, gate_weight, up_weight, down_weight, expert_ids, route_weight = (
        lax.optimization_barrier(
            (outgoing, gate_weight, up_weight, down_weight, expert_ids, route_weight)
        )
    )
    received = exchange(outgoing.reshape(EXPERTS, MOST, piece), "ep")
    received = received.reshape(capacity, piece)

    gate_up_near = shift(gate_up_piece(gate_weight, up_weight, target), 1)
    gate_up_far = swap(gate_up_near)
    down_near = shift(down_piece(down_weight, target), 1)
    down_far = swap(down_near)
    gate_up_here, down_here, half = cut_own(
        gate_weight, up_weight, down_weight, here, target_two, core
    )
    mine = hop_two(half)
    other = swap(mine)
    down_two = jnp.concatenate(
        [jnp.where(core == 0, mine, other), jnp.where(core == 0, other, mine)], 1
    )
    weights = weigh(expert_ids, route_weight)

    def product(weights):
        return jnp.dot(received, weights, preferred_element_type=jnp.float32)

    from_far = shift(product(gate_up_near).astype(jnp.bfloat16), -1)
    from_near = shift(product(gate_up_far).astype(jnp.bfloat16), 1)
    gate_up = product(gate_up_here)
    gate_up = gate_up + from_far.astype(jnp.float32) + from_near.astype(jnp.float32)
    hidden = (jax.nn.silu(gate_up[:, :units]) * gate_up[:, units:]).astype(jnp.bfloat16)
    hidden_two = hop_two(hidden)
    hidden_near = shift(hidden, 1)
    hidden_far = shift(hidden, -1)
    partial_rows = jnp.dot(
        jnp.concatenate([hidden_near, hidden, hidden_far, hidden_two], 1),
        jnp.concatenate([down_near, down_here, down_far, down_two], 0),
        preferred_element_type=jnp.float32,
    ).astype(jnp.bfloat16)
    size = width // BACK
    returned = exchange(partial_rows.reshape(EXPERTS, MOST, size), "ep")
    combined = combine(weights, returned.reshape(capacity, size)).astype(jnp.bfloat16)

    arrived = exchange(combined.reshape(tp_size, rows_here // tp_size, size), "tp")
    arrived = arrived.reshape(tp_size // BACK, BACK, rows_here // tp_size, size)
    arrived = sum(arrived[i].astype(jnp.float32) for i in range(tp_size // BACK))
    return jnp.concatenate([arrived[i] for i in range(BACK)], 1).astype(jnp.bfloat16)


def solution(mesh):
    in_specs = (
        P(("ep", "dp"), None),
        P(("ep", "dp"), None),
        P(("ep", "dp"), None),
        P("ep", None, "tp"),
        P("ep", None, "tp"),
        P("ep", "tp", None),
    )
    out_specs = P(("ep", "dp", "tp"), None)
    return jax.shard_map(
        per_device, mesh=mesh, in_specs=in_specs, out_specs=out_specs, check_vma=False
    )
```

```python
import jax
import jax.numpy as jnp
from jax import lax
from jax.experimental import pallas as pl
from jax.experimental.pallas import tpu as pltpu
from jax.sharding import PartitionSpec as P

TOP = 8
EXPERTS = 32
MOST = 8
LANES = 128
PARTS = 3
BACK = 4
STRIPS = 4
BLOCK = 5 * LANES


def shift(array, step):
    size = lax.axis_size("tp")
    pairs = [
        (core * size + i, core * size + (i + sign * step) % size)
        for core, sign in ((0, 1), (1, -1))
        for i in range(size)
    ]
    return lax.ppermute(array, ("dp", "tp"), pairs)


def swap(array):
    return lax.ppermute(array, "dp", [(0, 1), (1, 0)])


def exchange(array, axis):
    return lax.all_to_all(array, axis, split_axis=0, concat_axis=0, tiled=True)


def hop_two(array):
    size = lax.axis_size("tp")
    return lax.ppermute(
        array, "tp", [(i, (i + (2 if i % 2 else size - 2)) % size) for i in range(size)]
    )


def piece_width(width):
    tiles = -(-width // LANES)
    return -(-tiles // PARTS) * LANES


def piece_start(index, width):
    piece = piece_width(width)
    return jnp.minimum(lax.rem(index, PARTS) * piece, width - piece)


def cut_gate_up(start_ref, gate_ref, up_ref, out_ref, held, in_sem, out_sem):
    piece, units = out_ref.shape[0], gate_ref.shape[2]
    rows = piece // STRIPS
    arriving, leaving = [], []
    for strip in range(STRIPS):
        source = pl.ds(pl.multiple_of(start_ref[0] + strip * rows, 16), rows)
        target = pl.ds(strip * rows, rows)
        arriving.append(
            [
                pltpu.make_async_copy(
                    ref.at[0, source, :],
                    held.at[target, pl.ds(i * units, units)],
                    in_sem.at[strip, i],
                )
                for i, ref in enumerate((gate_ref, up_ref))
            ]
        )
        leaving.append(
            pltpu.make_async_copy(held.at[target, :], out_ref.at[target, :], out_sem.at[strip])
        )
    for pair in arriving:
        for copy in pair:
            copy.start()
    for pair, out in zip(arriving, leaving):
        for copy in pair:
            copy.wait()
        out.start()
    for out in leaving:
        out.wait()


def cut_down(start_ref, down_ref, out_ref, sem):
    columns = pl.ds(pl.multiple_of(start_ref[0], LANES), out_ref.shape[1])
    copy = pltpu.make_async_copy(down_ref.at[0, :, columns], out_ref, sem.at[0])
    copy.start()
    copy.wait()


def cut(kernel, start, arrays, shape, out_space, scratch):
    size = shape[0] * shape[1]
    return pl.pallas_call(
        kernel,
        out_shape=jax.ShapeDtypeStruct(shape, jnp.bfloat16),
        in_specs=[pl.BlockSpec(memory_space=pltpu.SMEM)]
        + [pl.BlockSpec(memory_space=pl.ANY)] * len(arrays),
        out_specs=pl.BlockSpec(memory_space=out_space),
        scratch_shapes=scratch,
        cost_estimate=pl.CostEstimate(
            flops=500 * size, bytes_accessed=4 * size, transcendentals=0
        ),
    )(start.reshape(1), *arrays)


def gate_up_piece(gate_weight, up_weight, index):
    width, units = gate_weight.shape[1:]
    shape = (piece_width(width), 2 * units)
    scratch = [
        pltpu.VMEM(shape, jnp.bfloat16),
        pltpu.SemaphoreType.DMA((STRIPS, 2)),
        pltpu.SemaphoreType.DMA((STRIPS,)),
    ]
    arrays = (gate_weight, up_weight)
    return cut(cut_gate_up, piece_start(index, width), arrays, shape, pl.ANY, scratch)


def down_piece(down_weight, index, half=None):
    units, width = down_weight.shape[1:]
    size = width // BACK
    start = lax.rem(index, BACK) * size
    if half is not None:
        size //= 2
        start = start + half * size
    scratch = [pltpu.SemaphoreType.DMA((1,))]
    return cut(cut_down, start, (down_weight,), (units, size), pltpu.VMEM, scratch)


def dispatch_kernel(start_ref, ids_ref, tokens_ref, rows_ref, ids, held, chosen, sem):
    capacity, count = chosen.shape
    width = tokens_ref.shape[1]
    piece = piece_width(width)
    block = rows_ref.shape[1]
    step = pl.program_id(0)

    @pl.when(step == 0)
    def _():
        ids_copy = pltpu.make_async_copy(ids_ref, ids, sem.at[1])
        ids_copy.start()
        start = pl.multiple_of(start_ref[0], LANES)
        copy = pltpu.make_async_copy(
            tokens_ref.at[:, pl.ds(start, piece)], held.at[:, pl.ds(0, piece)], sem.at[0]
        )
        copy.start()
        line = lax.broadcasted_iota(jnp.int32, (capacity, count), 0)
        expert, slot = line // MOST, line % MOST
        member = jnp.zeros((capacity, count), jnp.float32)
        ids_copy.wait()
        for k in range(TOP):
            member = jnp.where(ids[k : k + 1, :] == expert, 1.0, member)
        row = lax.broadcasted_iota(jnp.int32, (count, count), 0)
        column = lax.broadcasted_iota(jnp.int32, (count, count), 1)
        before = jnp.where(row < column, 1.0, 0.0).astype(jnp.bfloat16)
        earlier = jnp.dot(member.astype(jnp.bfloat16), before, preferred_element_type=jnp.float32)
        here = earlier == slot.astype(jnp.float32)
        chosen[...] = jnp.where(here, member, 0.0).astype(jnp.bfloat16)
        copy.wait()

    first = jnp.where(start_ref[0] == width - piece, PARTS * piece - width, 0)
    source = held[:, pl.ds(pl.multiple_of(step * block, LANES), block)]
    wide = lax.broadcasted_iota(jnp.int32, source.shape, 1) + step * block
    source = jnp.where(wide >= first, source.astype(jnp.float32), 0.0).astype(jnp.bfloat16)
    rows_ref[...] = jnp.dot(chosen[...], source, preferred_element_type=jnp.float32).astype(
        jnp.bfloat16
    )


def dispatch(tokens, expert_ids, index):
    count, width = tokens.shape
    piece, capacity = piece_width(width), EXPERTS * MOST
    steps = -(-piece // BLOCK)
    return pl.pallas_call(
        dispatch_kernel,
        grid=(steps,),
        out_shape=jax.ShapeDtypeStruct((capacity, piece), jnp.bfloat16),
        in_specs=[
            pl.BlockSpec(memory_space=pltpu.SMEM),
            pl.BlockSpec(memory_space=pl.ANY),
            pl.BlockSpec(memory_space=pl.ANY),
        ],
        out_specs=pl.BlockSpec((capacity, BLOCK), lambda i: (0, i)),
        scratch_shapes=[
            pltpu.VMEM((TOP, count), jnp.int32),
            pltpu.VMEM((count, steps * BLOCK), jnp.bfloat16),
            pltpu.VMEM((capacity, count), jnp.bfloat16),
            pltpu.SemaphoreType.DMA((2,)),
        ],
        cost_estimate=pl.CostEstimate(
            flops=2 * count * piece * capacity, bytes_accessed=2**21, transcendentals=0
        ),
        name="dispatch",
    )(piece_start(index, width).reshape(1), expert_ids.T, tokens)


def weigh_kernel(ids_ref, route_ref, weights_ref):
    capacity, count = weights_ref.shape[1:]
    line = lax.broadcasted_iota(jnp.int32, (capacity, count), 0)
    expert, slot = line // MOST, line % MOST
    member = jnp.zeros((capacity, count), jnp.float32)
    weight = jnp.zeros((capacity, count), jnp.float32)
    for k in range(TOP):
        same = ids_ref[k : k + 1, :] == expert
        member = jnp.where(same, 1.0, member)
        weight = jnp.where(same, route_ref[k : k + 1, :], weight)
    row = lax.broadcasted_iota(jnp.int32, (count, count), 0)
    column = lax.broadcasted_iota(jnp.int32, (count, count), 1)
    before = jnp.where(row < column, 1.0, 0.0).astype(jnp.bfloat16)
    earlier = jnp.dot(member.astype(jnp.bfloat16), before, preferred_element_type=jnp.float32)
    weight = jnp.where(earlier == slot.astype(jnp.float32), weight, 0.0)
    high = weight.astype(jnp.bfloat16)
    weights_ref[0] = high
    weights_ref[1] = (weight - high.astype(jnp.float32)).astype(jnp.bfloat16)


def weigh(expert_ids, route_weight):
    shape = (2, EXPERTS * MOST, expert_ids.shape[0])
    return pl.pallas_call(
        weigh_kernel,
        out_shape=jax.ShapeDtypeStruct(shape, jnp.bfloat16),
        cost_estimate=pl.CostEstimate(
            flops=2**26, bytes_accessed=2**15, transcendentals=0
        ),
        name="weigh",
    )(expert_ids.T, route_weight.T)


def combine(weights, returned):
    sums = jnp.einsum("ipt,pd->itd", weights, returned, preferred_element_type=jnp.float32)
    return sums[0] + sums[1]


def per_device(tokens, expert_ids, route_weight, gate_weight, up_weight, down_weight):
    rows_here, width = tokens.shape
    piece = piece_width(width)
    units = gate_weight.shape[2]
    capacity = EXPERTS * MOST
    tp_size = lax.axis_size("tp")
    here = lax.axis_index("tp")
    core = lax.axis_index("dp")
    target = lax.rem(here + jnp.where(core == 0, 1, tp_size - 1), tp_size)
    target_two = lax.rem(here + jnp.where(lax.rem(here, 2) == 0, tp_size - 2, 2), tp_size)

    outgoing = dispatch(tokens, expert_ids, here)
    outgoing, gate_weight, up_weight, down_weight, expert_ids, route_weight = (
        lax.optimization_barrier(
            (outgoing, gate_weight, up_weight, down_weight, expert_ids, route_weight)
        )
    )
    received = exchange(outgoing.reshape(EXPERTS, MOST, piece), "ep")
    received = received.reshape(capacity, piece)

    gate_up_near = shift(gate_up_piece(gate_weight, up_weight, target), 1)
    gate_up_far = swap(gate_up_near)
    down_near = shift(down_piece(down_weight, target), 1)
    down_far = swap(down_near)
    mine = hop_two(down_piece(down_weight, target_two, core))
    other = swap(mine)
    down_two = jnp.concatenate(
        [jnp.where(core == 0, mine, other), jnp.where(core == 0, other, mine)], 1
    )
    gate_up_here = gate_up_piece(gate_weight, up_weight, here)
    down_here = down_piece(down_weight, here)
    weights = weigh(expert_ids, route_weight)

    def product(weights):
        return jnp.dot(received, weights, preferred_element_type=jnp.float32)

    from_far = shift(product(gate_up_near).astype(jnp.bfloat16), -1)
    from_near = shift(product(gate_up_far).astype(jnp.bfloat16), 1)
    gate_up = product(gate_up_here)
    gate_up = gate_up + from_far.astype(jnp.float32) + from_near.astype(jnp.float32)
    hidden = (jax.nn.silu(gate_up[:, :units]) * gate_up[:, units:]).astype(jnp.bfloat16)
    hidden_two = hop_two(hidden)
    hidden_near = shift(hidden, 1)
    hidden_far = shift(hidden, -1)
    partial_rows = jnp.dot(
        jnp.concatenate([hidden_near, hidden, hidden_far, hidden_two], 1),
        jnp.concatenate([down_near, down_here, down_far, down_two], 0),
        preferred_element_type=jnp.float32,
    ).astype(jnp.bfloat16)
    size = width // BACK
    returned = exchange(partial_rows.reshape(EXPERTS, MOST, size), "ep")
    combined = combine(weights, returned.reshape(capacity, size)).astype(jnp.bfloat16)

    arrived = exchange(combined.reshape(tp_size, rows_here // tp_size, size), "tp")
    arrived = arrived.reshape(tp_size // BACK, BACK, rows_here // tp_size, size)
    arrived = sum(arrived[i].astype(jnp.float32) for i in range(tp_size // BACK))
    return jnp.concatenate([arrived[i] for i in range(BACK)], 1).astype(jnp.bfloat16)


def solution(mesh):
    in_specs = (
        P(("ep", "dp"), None),
        P(("ep", "dp"), None),
        P(("ep", "dp"), None),
        P("ep", None, "tp"),
        P("ep", None, "tp"),
        P("ep", "tp", None),
    )
    out_specs = P(("ep", "dp", "tp"), None)
    return jax.shard_map(
        per_device, mesh=mesh, in_specs=in_specs, out_specs=out_specs, check_vma=False
    )
```
